32 devices in a mesh: groups: 2 (over y), col: 16 (over z, x, core).
Axes of the slice: x: 2, y: 2, z: 4, core: 2. Of those that a mesh axis runs over, the one named last changes fastest.
Arguments:
- fields: bfloat16 [32, 137, 2048], P(('groups', 'col')), parts along dimension 0, may hold values from -6 to 6
- level_count: int32 [2048], replicated, may hold values from 68 to 137
- owner: int32 [16], replicated, may hold values from 0 to 15, as said below
- band_start: int32 [16, 37], replicated, may hold values from 0 to 133
- interp_weights: float32 [16, 37, 4], replicated, may hold values from -3 to 3
Outputs:
- timemajor: bfloat16 [32, 37, 2048], P(('groups', 'col')), parts along dimension 0
- series: bfloat16 [96, 37, 16, 128], P(('groups', 'col')), parts along dimension 0
The draws below stay inside these ranges and needn't reach their ends.
There are 2 independent parts, one for each index of `groups`. The reference program is written for one: setup_inputs(seed, part) draws one part's arguments, and reference() takes and returns one part's arrays. A program takes and returns all parts, laid end to end along the dimension named above; an argument that names none is the same for every part. Nothing has to cross between parts.
Inputs may be any that keep to these rules, and one draw needn't show every extreme that they name: No owner holds more than 3 blocks, and some owner holds exactly 3.
All inputs are finite; a program needn't handle non-finite values.
Results may differ from the reference program's by a relative error of at most 0.0085.
Values may be sent and summed in bfloat16 or wider, within the bound.
A program may use at most 64 MiB of HBM per device.

```python
import jax
import jax.numpy as jnp
from jax import lax

LEV = 137
PLEV = 37
BAND = 4
CBLK = 128
MOST = 3
TIMES = 16
BLOCKS = 16
COLS = 2048
N_COL = 16


def draw_owner(key, part):
    total = N_COL * MOST
    first, second, third = jax.random.split(jax.random.fold_in(key, 11), 3)
    chosen = jax.random.randint(first, (), 0, N_COL)
    order = jax.random.permutation(second, total).astype(jnp.int32)
    slot_index = jnp.arange(total, dtype=jnp.int32)
    slot_owner = slot_index // MOST
    at_ends = (slot_index == 0) | (slot_index == (N_COL - 1) * MOST)
    score = jnp.where(slot_owner == chosen, order - 3 * total, jnp.where(at_ends, order - 2 * total, order))
    picked = jnp.argsort(score, stable=True)[:N_COL]
    owners = (picked // MOST).astype(jnp.int32)
    shuffle = jax.random.permutation(third, N_COL)
    return owners[shuffle].astype(jnp.int32)


def set_ends(values, rng, low, high):
    longest = values.shape.index(max(values.shape))
    spots = []
    for shift in (0, 1):
        where = [jax.random.randint(jax.random.fold_in(rng, axis), (), 0, length) for axis, length in enumerate(values.shape)]
        where[longest] = (where[longest] + shift) % values.shape[longest]
        spots.append(tuple(where))
    return values.at[spots[0]].set(low).at[spots[1]].set(high)


def block_levels(stream_key, shape, cuts, low, top_value):
    def one(axis_at, parts):
        heights = jax.random.uniform(jax.random.fold_in(jax.random.fold_in(stream_key, 6), axis_at), (parts,), jnp.float32, low / len(cuts), top_value / len(cuts))
        return jnp.repeat(jnp.exp(heights), shape[axis_at] // parts).reshape((-1,) + (1,) * (len(shape) - axis_at - 1))

    factor_of = one(*cuts[0])
    for cut in cuts[1:]:
        factor_of = factor_of * one(*cut)
    return factor_of


def centred(key, shape, scale, limit, cuts=(), held_as=jnp.bfloat16):
    values = jax.random.normal(key, shape, jnp.float32) * scale
    if len(cuts) > 0:
        values = block_levels(key, shape, cuts, -0.22, 0.18) * values
    return jnp.clip(values, min=-limit, max=limit).astype(held_as)


def setup_inputs(seed: int = 0, part: int = 0) -> dict:
    arg_keys = jax.random.split(jax.random.key(seed), 6)
    part_keys = jax.random.split(jax.random.fold_in(arg_keys[5], part), 6)
    return {
        "fields": centred(part_keys[0], (TIMES, LEV, COLS), 1.0, 6.0, ((0, 16),)),
        "level_count": set_ends(jax.random.randint(arg_keys[1], (COLS,), LEV // 2, LEV + 1), jax.random.fold_in(arg_keys[1], 1), LEV // 2, LEV).astype(jnp.int32),
        "owner": draw_owner(jax.random.fold_in(arg_keys[5], 71), part),
        "band_start": set_ends(jax.random.randint(arg_keys[3], (BLOCKS, PLEV), 0, LEV - BAND + 1), jax.random.fold_in(arg_keys[3], 1), 0, LEV - BAND).astype(jnp.int32),
        "interp_weights": centred(arg_keys[4], (BLOCKS, PLEV, BAND), BAND ** -0.5, 3.0, (), jnp.float32),
    }


def fill_levels(block, counts):
    lev = jnp.arange(LEV, dtype=jnp.int32)[:, None]
    last = jnp.sum(jnp.where(lev == counts[None, :] - 1, block.astype(jnp.float32), 0.0), axis=1, keepdims=True)
    return jnp.where(lev < counts[None, :], block, last.astype(jnp.bfloat16))


def level_matrix(weights, starts):
    lev = jnp.arange(LEV, dtype=jnp.int32)
    offsets = jnp.arange(BAND, dtype=jnp.int32)
    hit = lev[None, None, :] == (starts[:, None] + offsets[None, :])[:, :, None]
    return jnp.sum(weights[:, :, None] * hit.astype(jnp.float32), axis=1).astype(jnp.bfloat16)


def reference(fields, level_count, owner, band_start, interp_weights):
    times = fields.shape[0]
    blocks = owner.shape[0]
    grouped = jnp.moveaxis(fields.reshape(times, LEV, blocks, CBLK), 2, 0)
    counts = level_count.reshape(blocks, CBLK)

    def one_block(items):
        block, count_row, weights, starts = items
        filled = fill_levels(block, count_row)
        matrix = level_matrix(weights, starts)
        result = jnp.einsum("pl,tlc->tpc", matrix.astype(jnp.float32), filled.astype(jnp.float32))
        return result.astype(jnp.bfloat16)

    results = lax.map(one_block, (grouped, counts, interp_weights, band_start))
    timemajor = jnp.moveaxis(results, 0, 2).reshape(times, PLEV, blocks * CBLK)
    onehot = (owner[:, None] == jnp.arange(N_COL, dtype=jnp.int32)[None, :]).astype(jnp.int32)
    before = jnp.cumsum(onehot, axis=0) - onehot
    slot = jnp.sum(before * onehot, axis=1).astype(jnp.int32)
    global_slot = (owner * MOST + slot).astype(jnp.int32)
    series = jnp.zeros((N_COL * MOST, PLEV, times, CBLK), jnp.bfloat16)
    series = series.at[global_slot].set(jnp.transpose(results, (0, 2, 1, 3)))
    return timemajor, series
```

```python
import functools

import jax
import jax.numpy as jnp
from jax import lax
from jax.experimental import pallas as pl
from jax.experimental.pallas import tpu as pltpu
from jax.sharding import PartitionSpec as P

LEV = 137
PLEV = 37
BAND = 4
CBLK = 128
MOST = 3
TILE = 16
LOW = (LEV // 2 - 1) // TILE * TILE
TALL = -(-LEV // TILE) * TILE
ROWS = -(-MOST * PLEV // TILE) * TILE
CHUNKS = 4
BANDS = 4
SEND = ((2, 1, 0, 3), (2, 3, 1, 0), (0, 1, 2, 3), (0, 2, 3, 1))
OWN = 2
TAKE = ((0, 1, 2, 3), (1, 0, 2, 3), (2, 3, 1, 0), (3, 2, 1, 0))


def loop(first, last, body):
    if last - first <= 16:
        for i in range(first, last):
            body(i)
    else:

        def step(i, carry):
            body(i)
            return carry

        lax.fori_loop(first, last, step, 0)


def choose(table, place, band):
    value = jnp.int32(table[0][place])
    for q in range(1, BANDS):
        value = jnp.where(band == q, jnp.int32(table[q][place]), value)
    return value


def kernel(n, blocks, fields, counts_in, owner_in, starts_in, weights_in, tm, series,
           data, counts, owner, starts, weights, start3, weight3, res, packed, arrived, wide,
           load_sem, small_sem, send_sem, recv_sem, ready):
    me = lax.axis_index("col")
    half = n // 2
    quarter = n // BANDS
    band = me // quarter
    seat = me % quarter
    barrier = pltpu.get_barrier_semaphore()

    smalls = []
    for i, (src, dst) in enumerate(
        [(owner_in, owner), (starts_in, starts), (weights_in, weights), (counts_in, counts)]
    ):
        small = pltpu.make_async_copy(src, dst, small_sem.at[i])
        small.start()
        smalls.append(small)
    width = data.shape[1] // CHUNKS
    loads = []
    for i in range(CHUNKS):
        span = pl.ds(i * width, width)
        load = pltpu.make_async_copy(
            fields.at[0, :, span], data.at[:, span], load_sem.at[i]
        )
        load.start()
        loads.append(load)

    other = (1 - me // half) * half

    def greet(i):
        pl.semaphore_signal(
            barrier, inc=1, device_id={"col": other + (me + i) % half},
            device_id_type=pl.DeviceIdType.MESH,
        )

    loop(0, half, greet)

    res[blocks] = jnp.zeros(res.shape[1:], jnp.bfloat16)
    for small in smalls:
        small.wait()

    start3[...] = jnp.concatenate(
        [starts[...].astype(jnp.float32)] * MOST
        + [jnp.full((blocks, CBLK - MOST * PLEV), -float(CBLK), jnp.float32)], axis=1)
    weight3[...] = jnp.concatenate(
        [weights[...]] * MOST
        + [jnp.zeros((blocks * BAND, CBLK - MOST * PLEV), jnp.float32)], axis=1)

    row = lax.broadcasted_iota(jnp.int32, (TILE, CBLK), 0).astype(jnp.float32).astype(jnp.bfloat16)

    def packed_row(ref, i):
        return jnp.broadcast_to(ref[pl.ds(i, 1), :], (TILE, CBLK)).astype(jnp.bfloat16)

    def interpolate(b):
        cols = pl.ds(pl.multiple_of(b * CBLK, CBLK), CBLK)
        zero = jnp.zeros((TILE, CBLK), jnp.bfloat16)
        count = jnp.broadcast_to(
            counts[pl.ds(b, 1), :].astype(jnp.float32), (TILE, CBLK)).astype(jnp.bfloat16)
        first = packed_row(start3, b)
        terms = [packed_row(weight3, b * BAND + k) for k in range(BAND)]
        filled = [data[:LOW, cols]]
        last = zero
        ends = 0.0
        for i in range(LOW, LEV, TILE):
            size = min(TILE, LEV - i)
            part = jnp.where(row[:size] + float(i + 1) == count[:size], data[i:i + size, cols], zero[:size])
            if size == TILE:
                last = last + part
            else:
                ends = jnp.sum(part.astype(jnp.float32), axis=0, keepdims=True)
        last = jnp.sum(last.astype(jnp.float32), axis=0, keepdims=True) + ends
        last = jnp.broadcast_to(last, (TILE, CBLK)).astype(jnp.bfloat16)
        for i in range(LOW, LEV, TILE):
            size = min(TILE, LEV - i)
            filled.append(jnp.where(row[:size] + float(i) < count[:size], data[i:i + size, cols], last[:size]))
        matrix = []
        for i in range(0, LEV, TILE):
            size = min(TILE, LEV - i)
            offset = (row[:size] + float(i)) - first[:size]
            part = zero[:size]
            for k in range(BAND):
                part = jnp.where(offset == float(k), terms[k][:size], part)
            matrix.append(part)
        out = lax.dot_general(
            jnp.concatenate(matrix, axis=0), jnp.concatenate(filled, axis=0),
            (((0,), (0,)), ((), ())), preferred_element_type=jnp.float32,
        )
        out = out[:ROWS].astype(jnp.bfloat16)
        res[b] = out
        tm[0, :, cols] = out[:PLEV]

    per = blocks // CHUNKS
    for i in range(CHUNKS):
        loads[i].wait()
        loop(i * per, (i + 1) * per, interpolate)

    unit = 1 << blocks.bit_length()

    def find(d):
        def look(i, found):
            b = blocks - 1 - i
            return jnp.where(owner[b] == d, found * unit + b, found)

        found = jnp.int32(blocks)
        for s in range(1, MOST):
            found = found * unit + blocks
        if blocks <= 16:
            for i in range(blocks):
                found = look(i, found)
        else:
            found = lax.fori_loop(0, blocks, look, found)
        return [(found // unit ** s) % unit for s in range(MOST)]

    def pack(k, d):
        where = find(d)
        for i in range(0, ROWS, TILE):
            slots = [s for s in range(MOST) if s * PLEV < i + TILE and (s + 1) * PLEV > i]
            part = res[where[slots[0]], pl.ds(i, TILE)]
            for s in slots[1:]:
                part = jnp.where(
                    row < float(s * PLEV - i), part, res[where[s], pl.ds(i, TILE)])
            packed[k, pl.ds(i, TILE)] = part

    def copy(k, src_dst, slot):
        return pltpu.make_async_remote_copy(
            src_ref=packed.at[k], dst_ref=arrived.at[slot],
            send_sem=send_sem.at[k], recv_sem=recv_sem.at[slot],
            device_id={"col": src_dst}, device_id_type=pl.DeviceIdType.MESH,
        )

    def target(place, j):
        return choose(SEND, place, band) * quarter + (seat + j) % quarter

    def send_band(place):
        def one(j):
            pack(place * quarter + j, target(place, j))

            @pl.when(j > 0)
            def _():
                copy(place * quarter + j - 1, target(place, j - 1), me).start()

        if place != OWN:
            if quarter <= 16:
                for j in range(quarter):
                    pack(place * quarter + j, target(place, j))
                    if j:
                        copy(place * quarter + j - 1, target(place, j - 1), me).start()
            else:
                loop(0, quarter, one)
            copy((place + 1) * quarter - 1, target(place, quarter - 1), me).start()
        else:
            def local(j):
                pack(place * quarter + j, target(place, j))

            loop(0, quarter, local)

            def send(j):
                copy(place * quarter + j, target(place, j), me).start()

            loop(1, quarter, send)

    pl.semaphore_wait(barrier, half)
    pl.semaphore_signal(
        ready, inc=1, device_id={"col": (me + half) % n}, device_id_type=pl.DeviceIdType.MESH)
    send_band(0)
    pl.semaphore_wait(ready, 1)
    for place in range(1, BANDS):
        send_band(place)

    def spread(t, rows):
        wide[:, pl.ds(t, 1), :] = rows.astype(jnp.float32)[:, None, :]

    spread(me, packed[OWN * quarter])

    def take(place):
        def one(j):
            src = choose(TAKE, place, band) * quarter + (seat + quarter - j) % quarter
            copy(0, src, src).wait_recv()
            spread(src, arrived[src])

        loop(1 if place == 0 else 0, quarter, one)

    for place in range(BANDS):
        take(place)
    for s in range(MOST):
        series[s] = wide[s * PLEV:(s + 1) * PLEV].astype(jnp.bfloat16)

    def sent(k):
        copy(k, me, me).wait_send()

    loop(0, OWN * quarter, sent)
    loop(OWN * quarter + 1, n, sent)


def close(tm, series, tm_out, series_out, sems):
    first = pltpu.make_async_copy(series, series_out, sems.at[0])
    second = pltpu.make_async_copy(tm, tm_out, sems.at[1])
    first.start()
    second.start()
    first.wait()
    second.wait()


def per_device(fields, level_count, owner, band_start, interp_weights):
    n = lax.axis_size("col")
    blocks = owner.shape[0]
    anywhere = pl.BlockSpec(memory_space=pl.ANY)
    cols = blocks * CBLK
    vmem = pl.BlockSpec(memory_space=pltpu.VMEM)
    grant = 2 * cols * TALL + 2 * CBLK * ROWS * (blocks + 1 + 2 * n) + 4 * CBLK * n * ROWS
    grant += blocks * CBLK * 4 * 16 + 2 * cols * 48 + 2 * n * ROWS * CBLK + (3 << 20)
    timemajor, series = pl.pallas_call(
        functools.partial(kernel, n, blocks),
        out_shape=(
            jax.ShapeDtypeStruct((1, PLEV, cols), jnp.bfloat16),
            jax.ShapeDtypeStruct((MOST, PLEV, n, CBLK), jnp.bfloat16),
        ),
        in_specs=[pl.BlockSpec(memory_space=pltpu.HBM)] * 5,
        out_specs=(vmem, vmem),
        scratch_shapes=[
            pltpu.VMEM((LEV, cols), jnp.bfloat16),
            pltpu.VMEM((blocks, CBLK), jnp.int32),
            pltpu.SMEM((blocks,), jnp.int32),
            pltpu.VMEM((blocks, PLEV), jnp.int32),
            pltpu.VMEM((blocks * BAND, PLEV), jnp.float32),
            pltpu.VMEM((blocks, CBLK), jnp.float32),
            pltpu.VMEM((blocks * BAND, CBLK), jnp.float32),
            pltpu.VMEM((blocks + 1, ROWS, CBLK), jnp.bfloat16),
            pltpu.VMEM((n, ROWS, CBLK), jnp.bfloat16),
            pltpu.VMEM((n, ROWS, CBLK), jnp.bfloat16),
            pltpu.VMEM((ROWS, n, CBLK), jnp.float32),
            pltpu.SemaphoreType.DMA((CHUNKS,)),
            pltpu.SemaphoreType.DMA((4,)),
            pltpu.SemaphoreType.DMA((n,)),
            pltpu.SemaphoreType.DMA((n,)),
            pltpu.SemaphoreType.REGULAR,
        ],
        compiler_params=pltpu.CompilerParams(
            collective_id=0, has_side_effects=True, vmem_limit_bytes=grant
        ),
    )(
        *[pltpu.with_memory_space_constraint(x, pltpu.HBM) for x in (
            fields, level_count.reshape(blocks, CBLK), owner, band_start,
            jnp.swapaxes(interp_weights, 1, 2).reshape(blocks * BAND, PLEV),
        )]
    )
    return pl.pallas_call(
        close,
        out_shape=(
            jax.ShapeDtypeStruct((1, PLEV, cols), jnp.bfloat16),
            jax.ShapeDtypeStruct((MOST, PLEV, n, CBLK), jnp.bfloat16),
        ),
        in_specs=[vmem, vmem],
        out_specs=(anywhere, anywhere),
        scratch_shapes=[pltpu.SemaphoreType.DMA((2,))],
        compiler_params=pltpu.CompilerParams(vmem_limit_bytes=3 << 20),
    )(timemajor, series)


def solution(mesh):
    placed = (P(("groups", "col"), None, None), P(), P(), P(), P())
    return jax.shard_map(
        per_device,
        mesh=mesh,
        in_specs=placed,
        out_specs=(P(("groups", "col"), None, None), P(("groups", "col"), None, None, None)),
        check_vma=False,
    )
```

```python
import functools

import jax
import jax.numpy as jnp
from jax import lax
from jax.experimental import pallas as pl
from jax.experimental.pallas import tpu as pltpu
from jax.sharding import PartitionSpec as P

LEV = 137
PLEV = 37
BAND = 4
CBLK = 128
MOST = 3
TILE = 16
LOW = (LEV // 2 - 1) // TILE * TILE
TALL = -(-LEV // TILE) * TILE
ROWS = -(-MOST * PLEV // TILE) * TILE
WIDE = -(-PLEV // TILE) * TILE
BANDS = 4
SEND = ((1, 0, 2, 3), (2, 1, 0, 3), (0, 2, 1, 3), (0, 3, 2, 1))
OWN = 1
TAKE = ((0, 1, 2, 3), (1, 0, 2, 3), (2, 3, 1, 0), (3, 2, 1, 0))


def loop(first, last, body):
    if last - first <= 16:
        for i in range(first, last):
            body(i)
    else:

        def step(i, carry):
            body(i)
            return carry

        lax.fori_loop(first, last, step, 0)


def choose(table, place, band):
    value = jnp.int32(table[0][place])
    for q in range(1, BANDS):
        value = jnp.where(band == q, jnp.int32(table[q][place]), value)
    return value


def kernel(n, blocks, fields, counts_in, owner_in, starts_in, weights_in, tm, series,
           data, counts, owner, starts, weights, start_row, weight_row, matrix, res, packed, arrived, wide,
           load_sem, small_sem, send_sem, recv_sem, near, far):
    me = lax.axis_index("col")
    half = n // 2
    quarter = n // BANDS
    band = me // quarter
    seat = me % quarter
    barrier = pltpu.get_barrier_semaphore()

    smalls = []
    for i, (src, dst) in enumerate(
        [(owner_in, owner), (starts_in, starts), (weights_in, weights), (counts_in, counts)]
    ):
        small = pltpu.make_async_copy(src, dst, small_sem.at[i])
        small.start()
        smalls.append(small)
    load = pltpu.make_async_copy(fields.at[0], data, load_sem)
    load.start()

    def greet(d):
        pl.semaphore_signal(
            barrier, inc=1, device_id={"col": d}, device_id_type=pl.DeviceIdType.MESH)

    @pl.when(band < 2)
    def _():
        loop(1, n, lambda i: greet((me + i) % n))

    @pl.when(band == 2)
    def _():
        loop(0, quarter, lambda i: greet(quarter + i))
        loop(1, quarter, lambda i: greet(half + (seat + i) % quarter))
        loop(0, quarter, lambda i: greet(half + quarter + i))

    @pl.when(band == 3)
    def _():
        loop(1, quarter, lambda i: greet(half + quarter + (seat + i) % quarter))

    res[blocks] = jnp.zeros(res.shape[1:], jnp.bfloat16)
    for small in smalls[:-1]:
        small.wait()

    start_row[...] = jnp.concatenate(
        [starts[...].astype(jnp.float32),
         jnp.full((blocks, CBLK - PLEV), -float(CBLK), jnp.float32)], axis=1)
    weight_row[...] = jnp.concatenate(
        [weights[...], jnp.zeros((blocks * BAND, CBLK - PLEV), jnp.float32)], axis=1)

    unit = 1 << blocks.bit_length()

    def find(d):
        def look(i, found):
            b = blocks - 1 - i
            return jnp.where(owner[b] == d, found * unit + b, found)

        found = jnp.int32(blocks)
        for s in range(1, MOST):
            found = found * unit + blocks
        if blocks <= 16:
            for i in range(blocks):
                found = look(i, found)
        else:
            found = lax.fori_loop(0, blocks, look, found)
        return [(found // unit ** s) % unit for s in range(MOST)]

    def target(place, j):
        return choose(SEND, place, band) * quarter + ((seat + j) % quarter if place == OWN else j)

    early = [find(target(0, j)) for j in range(quarter)] if quarter <= 16 else None

    row = lax.broadcasted_iota(jnp.int32, (TILE, CBLK), 0).astype(jnp.float32).astype(jnp.bfloat16)
    zero = jnp.zeros((TILE, CBLK), jnp.bfloat16)

    def packed_row(ref, i):
        return jnp.broadcast_to(ref[pl.ds(i, 1), :], (TILE, CBLK)).astype(jnp.bfloat16)

    def build(b):
        first = packed_row(start_row, b)
        terms = [packed_row(weight_row, b * BAND + k) for k in range(BAND)]
        parts = []
        for i in range(0, TALL, TILE):
            offset = (row + float(i)) - first
            part = zero
            for k in range(BAND):
                part = jnp.where(offset == float(k), terms[k], part)
            parts.append(part)
        matrix[b] = jnp.concatenate(parts, axis=0).T[:WIDE, :LEV]

    loop(0, blocks, build)

    def interpolate(b):
        cols = pl.ds(pl.multiple_of(b * CBLK, CBLK), CBLK)
        count = jnp.broadcast_to(
            counts[pl.ds(b, 1), :].astype(jnp.float32), (TILE, CBLK)).astype(jnp.bfloat16)
        filled = [data[:LOW, cols]]
        last = zero
        ends = 0.0
        for i in range(LOW, LEV, TILE):
            size = min(TILE, LEV - i)
            part = jnp.where(row[:size] + float(i + 1) == count[:size], data[i:i + size, cols], zero[:size])
            if size == TILE:
                last = last + part
            else:
                ends = jnp.sum(part.astype(jnp.float32), axis=0, keepdims=True)
        last = jnp.sum(last.astype(jnp.float32), axis=0, keepdims=True) + ends
        last = jnp.broadcast_to(last, (TILE, CBLK)).astype(jnp.bfloat16)
        for i in range(LOW, LEV, TILE):
            size = min(TILE, LEV - i)
            filled.append(jnp.where(row[:size] + float(i) < count[:size], data[i:i + size, cols], last[:size]))
        out = jnp.dot(
            matrix[b], jnp.concatenate(filled, axis=0), preferred_element_type=jnp.float32)[:PLEV]
        tm[0, :, cols] = out.astype(jnp.bfloat16)
        res[b] = jnp.concatenate(
            [out] * MOST + [jnp.zeros((ROWS - MOST * PLEV, CBLK), jnp.float32)], axis=0,
        ).astype(jnp.bfloat16)

    for small in smalls[-1:]:
        small.wait()
    load.wait()
    loop(0, blocks, interpolate)

    def pack(k, d, where=None):
        where = find(d) if where is None else where
        for i in range(0, ROWS, TILE):
            slots = [s for s in range(MOST) if s * PLEV < i + TILE and (s + 1) * PLEV > i]
            part = res[where[slots[0]], pl.ds(i, TILE)]
            for s in slots[1:]:
                part = jnp.where(
                    row < float(s * PLEV - i), part, res[where[s], pl.ds(i, TILE)])
            packed[k, pl.ds(i, TILE)] = part

    def copy(k, src_dst, slot):
        return pltpu.make_async_remote_copy(
            src_ref=packed.at[k], dst_ref=arrived.at[slot],
            send_sem=send_sem.at[k], recv_sem=recv_sem.at[slot],
            device_id={"col": src_dst}, device_id_type=pl.DeviceIdType.MESH,
        )

    def send_band(place):
        def one(j):
            pack(place * quarter + j, target(place, j))

            @pl.when(j > 0)
            def _():
                copy(place * quarter + j - 1, target(place, j - 1), me).start()

        if place != OWN:
            if quarter <= 16:
                for j in range(quarter):
                    pack(place * quarter + j, target(place, j), None if place else early[j])
                    if j:
                        copy(place * quarter + j - 1, target(place, j - 1), me).start()
            else:
                loop(0, quarter, one)
            copy((place + 1) * quarter - 1, target(place, quarter - 1), me).start()
        else:
            def local(j):
                pack(place * quarter + j, target(place, j))

            loop(0, quarter, local)

            def send(j):
                copy(place * quarter + j, target(place, j), me).start()

            loop(1, quarter, send)

    def tell(semaphore, d):
        pl.semaphore_signal(
            semaphore, inc=1, device_id={"col": d}, device_id_type=pl.DeviceIdType.MESH)

    for q in range(BANDS):
        @pl.when(band == q)
        def _(q=q):
            pl.semaphore_wait(barrier, (2, 3, 3, 4)[q] * quarter - 1)
            if q == 1:
                tell(near, me - quarter)
            if q == 3:
                for away in range(1, BANDS):
                    tell(far, me - away * quarter)

    send_band(0)
    send_band(1)

    @pl.when(band == 0)
    def _():
        pl.semaphore_wait(near, 1)

    send_band(2)

    @pl.when(band < 3)
    def _():
        pl.semaphore_wait(far, 1)

    send_band(3)

    def spread(t, rows):
        wide[:, pl.ds(t, 1), :] = rows.astype(jnp.float32)[:, None, :]

    spread(me, packed[OWN * quarter])

    def take(place):
        def one(j):
            src = choose(TAKE, place, band) * quarter + ((seat + quarter - j) % quarter if place == 0 else j)
            copy(0, src, src).wait_recv()
            spread(src, arrived[src])

        loop(1 if place == 0 else 0, quarter, one)

    for place in range(BANDS):
        take(place)
    for s in range(MOST):
        series[s] = wide[s * PLEV:(s + 1) * PLEV].astype(jnp.bfloat16)

    def sent(k):
        copy(k, me, me).wait_send()

    loop(0, OWN * quarter, sent)
    loop(OWN * quarter + 1, n, sent)


def close(tm, series, tm_out, series_out, sems):
    first = pltpu.make_async_copy(series, series_out, sems.at[0])
    second = pltpu.make_async_copy(tm, tm_out, sems.at[1])
    first.start()
    second.start()
    first.wait()
    second.wait()


def per_device(fields, level_count, owner, band_start, interp_weights):
    n = lax.axis_size("col")
    blocks = owner.shape[0]
    anywhere = pl.BlockSpec(memory_space=pl.ANY)
    cols = blocks * CBLK
    vmem = pl.BlockSpec(memory_space=pltpu.VMEM)
    grant = 2 * cols * TALL + 2 * CBLK * ROWS * (blocks + 1 + 2 * n) + 4 * CBLK * n * ROWS
    grant += blocks * CBLK * 4 * 16 + 2 * cols * 48 + 2 * n * ROWS * CBLK + blocks * WIDE * 512 + (3 << 20)
    timemajor, series = pl.pallas_call(
        functools.partial(kernel, n, blocks),
        out_shape=(
            jax.ShapeDtypeStruct((1, PLEV, cols), jnp.bfloat16),
            jax.ShapeDtypeStruct((MOST, PLEV, n, CBLK), jnp.bfloat16),
        ),
        in_specs=[pl.BlockSpec(memory_space=pltpu.HBM)] * 5,
        out_specs=(vmem, vmem),
        scratch_shapes=[
            pltpu.VMEM((LEV, cols), jnp.bfloat16),
            pltpu.VMEM((blocks, CBLK), jnp.int32),
            pltpu.SMEM((blocks,), jnp.int32),
            pltpu.VMEM((blocks, PLEV), jnp.int32),
            pltpu.VMEM((blocks * BAND, PLEV), jnp.float32),
            pltpu.VMEM((blocks, CBLK), jnp.float32),
            pltpu.VMEM((blocks * BAND, CBLK), jnp.float32),
            pltpu.VMEM((blocks, WIDE, LEV), jnp.bfloat16),
            pltpu.VMEM((blocks + 1, ROWS, CBLK), jnp.bfloat16),
            pltpu.VMEM((n, ROWS, CBLK), jnp.bfloat16),
            pltpu.VMEM((n, ROWS, CBLK), jnp.bfloat16),
            pltpu.VMEM((ROWS, n, CBLK), jnp.float32),
            pltpu.SemaphoreType.DMA,
            pltpu.SemaphoreType.DMA((4,)),
            pltpu.SemaphoreType.DMA((n,)),
            pltpu.SemaphoreType.DMA((n,)),
            pltpu.SemaphoreType.REGULAR,
            pltpu.SemaphoreType.REGULAR,
        ],
        compiler_params=pltpu.CompilerParams(
            collective_id=0, has_side_effects=True, vmem_limit_bytes=grant
        ),
    )(
        *[pltpu.with_memory_space_constraint(x, pltpu.HBM) for x in (
            fields, level_count.reshape(blocks, CBLK), owner, band_start,
            jnp.swapaxes(interp_weights, 1, 2).reshape(blocks * BAND, PLEV),
        )]
    )
    return pl.pallas_call(
        close,
        out_shape=(
            jax.ShapeDtypeStruct((1, PLEV, cols), jnp.bfloat16),
            jax.ShapeDtypeStruct((MOST, PLEV, n, CBLK), jnp.bfloat16),
        ),
        in_specs=[vmem, vmem],
        out_specs=(anywhere, anywhere),
        scratch_shapes=[pltpu.SemaphoreType.DMA((2,))],
        compiler_params=pltpu.CompilerParams(vmem_limit_bytes=3 << 20),
    )(timemajor, series)


def solution(mesh):
    placed = (P(("groups", "col"), None, None), P(), P(), P(), P())
    return jax.shard_map(
        per_device,
        mesh=mesh,
        in_specs=placed,
        out_specs=(P(("groups", "col"), None, None), P(("groups", "col"), None, None, None)),
        check_vma=False,
    )
```

```python
import functools

import jax
import jax.numpy as jnp
from jax import lax
from jax.experimental import pallas as pl
from jax.experimental.pallas import tpu as pltpu
from jax.sharding import PartitionSpec as P

LEV = 137
PLEV = 37
BAND = 4
CBLK = 128
MOST = 3
TILE = 16
LOW = (LEV // 2 - 1) // TILE * TILE
TALL = -(-LEV // TILE) * TILE
ROWS = -(-MOST * PLEV // TILE) * TILE
WIDE = -(-PLEV // TILE) * TILE
BANDS = 4
SEND = ((1, 2, 0, 3), (2, 0, 1, 3), (0, 1, 2, 3), (0, 2, 3, 1))
OWN = 2
OWN_AT = 1
CUTS = (0, 16)
EARLY = 2
STAGES = (0, 2, 4, 1 << 20)
STEPS = len(STAGES) - 1
EDGE = ((1, 0, 2, 3), (2, 3, 0, 1))
EDGE_TAKE = ((0, 1, 3, 2), (3, 2, 0, 1))
CROSS = (((3, 0), (3, 1), (3, 2), (3, 3), (2, 0), (2, 1), (2, 2), (2, 3)),
         ((0, 0), (0, 1), (0, 2), (0, 3), (1, 0), (1, 1), (1, 2), (1, 3)))
TAKE = ((0, 3, 2, 1), (1, 0, 3, 2), (2, 3, 0, 1), (3, 2, 0, 1))


def loop(first, last, body):
    if last - first <= 16:
        for i in range(first, last):
            body(i)
    else:

        def step(i, carry):
            body(i)
            return carry

        lax.fori_loop(first, last, step, 0)


def choose(table, place, band):
    value = jnp.int32(table[0][place])
    for q in range(1, BANDS):
        value = jnp.where(band == q, jnp.int32(table[q][place]), value)
    return value


def kernel(n, blocks, fields, counts_in, owner_in, starts_in, weights_in, tm, series,
           data, counts, owner, starts, weights, start_row, weight_row, matrix, res, packed, arrived, wide,
           load_sem, small_sem, send_sem, recv_sem, near, far, queued, again, queue_sem, again_sem, *lists):
    me = lax.axis_index("col")
    half = n // 2
    quarter = n // BANDS
    band = me // quarter
    seat = me % quarter
    barrier = pltpu.get_barrier_semaphore()

    smalls = []
    for i, (src, dst) in enumerate(
        [(owner_in, owner), (starts_in, starts), (weights_in, weights), (counts_in, counts)]
    ):
        small = pltpu.make_async_copy(src, dst, small_sem.at[i])
        small.start()
        smalls.append(small)
    loads = []
    for i, (first, last) in enumerate(zip(CUTS, CUTS[1:])):
        span = pl.ds(blocks * first // 16 * CBLK, blocks * (last - first) // 16 * CBLK)
        load = pltpu.make_async_copy(fields.at[0, :, span], data.at[:, span], load_sem.at[i])
        load.start()
        loads.append(load)

    def greet(d):
        pl.semaphore_signal(
            barrier, inc=1, device_id={"col": d}, device_id_type=pl.DeviceIdType.MESH)

    @pl.when(band < 2)
    def _():
        loop(1, n, lambda i: greet((me + i) % n))

    @pl.when(band == 2)
    def _():
        loop(0, quarter, lambda i: greet(quarter + i))
        loop(0, quarter, lambda i: greet(half + quarter + i))

    @pl.when(band == 3)
    def _():
        loop(1, quarter, lambda i: greet(half + quarter + (seat + i) % quarter))

    res[blocks] = jnp.zeros(res.shape[1:], jnp.bfloat16)
    for part in lists:
        part[part.shape[0] - 1] = jnp.zeros(part.shape[1:], jnp.bfloat16)
    for small in smalls[:-1]:
        small.wait()

    start_row[...] = jnp.concatenate(
        [starts[...].astype(jnp.float32),
         jnp.full((blocks, CBLK - PLEV), -float(CBLK), jnp.float32)], axis=1)
    weight_row[...] = jnp.concatenate(
        [weights[...], jnp.zeros((blocks * BAND, CBLK - PLEV), jnp.float32)], axis=1)

    unit = 1 << blocks.bit_length()
    relayed = blocks <= 16 and quarter <= 16
    groups = -(-blocks // MOST)

    def third(x):
        return (x * 43) >> 7

    def shift(c, turn):
        return jnp.where(c + turn >= MOST, c + turn - MOST, c + turn)

    if relayed:
        lower = jnp.int32(0)
        for b in range(blocks):
            lower = lower + jnp.where(owner[b] < half, 1, 0)

    def before(d):
        if not relayed:
            return jnp.int32(0)
        count = jnp.int32(0)
        for b in range(blocks):
            count = count + jnp.where(owner[b] < d, 1, 0)
        return count - jnp.where(d >= half, lower, 0)

    def find(d):
        def look(i, found):
            b = blocks - 1 - i
            return jnp.where(owner[b] == d, found * unit + b, found)

        found = jnp.int32(blocks)
        for s in range(1, MOST):
            found = found * unit + blocks
        if blocks <= 16:
            for i in range(blocks):
                found = look(i, found)
        else:
            found = lax.fori_loop(0, blocks, look, found)
        found = [(found // unit ** s) % unit for s in range(MOST)]
        if relayed:
            first = before(d)
            turn = first - MOST * third(first)
            found = [
                jnp.where(turn == 0, found[c], jnp.where(turn == 1, found[(c + 2) % 3], found[(c + 1) % 3]))
                for c in range(MOST)
            ]
        return found

    def locate(d):
        first = before(d)
        last = first
        for b in range(blocks):
            last = last + jnp.where(owner[b] == d, 1, 0)
        turn = first - MOST * third(first)
        where = []
        for c in range(MOST):
            place = first + jnp.where(c >= turn, c - turn, c - turn + MOST)
            where.append(jnp.where(place < last, third(place), groups))
        return where

    def ordered(base):
        keys = []
        for b in range(blocks):
            away = owner[b] - base
            keys.append(jnp.where(away < 0, away + n, away) * unit + b)
        size = 1 << (blocks - 1).bit_length()
        keys += [jnp.int32(n * unit + blocks)] * (size - blocks)
        p = 1
        while p < size:
            k = p
            while k >= 1:
                for j in range(k % p, size - k, 2 * k):
                    for i in range(min(k, size - j - k)):
                        if (i + j) // (2 * p) == (i + j + k) // (2 * p):
                            x, y = keys[i + j], keys[i + j + k]
                            keys[i + j], keys[i + j + k] = jnp.minimum(x, y), jnp.maximum(x, y)
                k //= 2
            p *= 2
        keys = [key % unit for key in keys[:blocks]]
        return keys + [jnp.int32(blocks)] * (groups * MOST - blocks)

    def target(place, j):
        return choose(SEND, place, band) * quarter + ((seat + j) % quarter if place == OWN else j)

    early = None
    if relayed:
        queue = ordered((1 - me // half) * half)
        inner = (band == 1) | (band == 2)
    elif quarter <= 16:
        early = [find(target(0, j)) for j in range(quarter)]

    row = lax.broadcasted_iota(jnp.int32, (TILE, CBLK), 0).astype(jnp.float32).astype(jnp.bfloat16)
    zero = jnp.zeros((TILE, CBLK), jnp.bfloat16)

    def packed_row(ref, i):
        return jnp.broadcast_to(ref[pl.ds(i, 1), :], (TILE, CBLK)).astype(jnp.bfloat16)

    def build(b):
        first = packed_row(start_row, b)
        terms = [packed_row(weight_row, b * BAND + k) for k in range(BAND)]
        parts = []
        for i in range(0, TALL, TILE):
            offset = (row + float(i)) - first
            part = zero
            for k in range(BAND):
                part = jnp.where(offset == float(k), terms[k], part)
            parts.append(part)
        matrix[b] = jnp.concatenate(parts, axis=0).T[:WIDE, :LEV]

    loop(0, blocks, build)

    def interpolate(b):
        cols = pl.ds(pl.multiple_of(b * CBLK, CBLK), CBLK)
        count = jnp.broadcast_to(
            counts[pl.ds(b, 1), :].astype(jnp.float32), (TILE, CBLK)).astype(jnp.bfloat16)
        filled = [data[:LOW, cols]]
        last = zero
        ends = 0.0
        for i in range(LOW, LEV, TILE):
            size = min(TILE, LEV - i)
            part = jnp.where(row[:size] + float(i + 1) == count[:size], data[i:i + size, cols], zero[:size])
            if size == TILE:
                last = last + part
            else:
                ends = jnp.sum(part.astype(jnp.float32), axis=0, keepdims=True)
        last = jnp.sum(last.astype(jnp.float32), axis=0, keepdims=True) + ends
        last = jnp.broadcast_to(last, (TILE, CBLK)).astype(jnp.bfloat16)
        for i in range(LOW, LEV, TILE):
            size = min(TILE, LEV - i)
            filled.append(jnp.where(row[:size] + float(i) < count[:size], data[i:i + size, cols], last[:size]))
        out = jnp.dot(
            matrix[b], jnp.concatenate(filled, axis=0), preferred_element_type=jnp.float32)[:PLEV]
        tm[0, :, cols] = out.astype(jnp.bfloat16)
        res[b] = jnp.concatenate(
            [out] * MOST + [jnp.zeros((ROWS - MOST * PLEV, CBLK), jnp.float32)], axis=0,
        ).astype(jnp.bfloat16)

    for small in smalls[-1:]:
        small.wait()
    for load, first, last in zip(loads, CUTS, CUTS[1:]):
        load.wait()
        loop(blocks * first // 16, blocks * last // 16, interpolate)

    def fill(target, source, where, rows=ROWS):
        for i in range(0, rows, TILE):
            slots = [s for s in range(MOST) if s * PLEV < i + TILE and (s + 1) * PLEV > i]
            part = source[where[slots[0]], pl.ds(i, TILE)]
            for s in slots[1:]:
                part = jnp.where(
                    row < float(s * PLEV - i), part, source[where[s], pl.ds(i, TILE)])
            target[pl.ds(i, TILE)] = part

    def pack(k, d, where=None):
        fill(packed.at[k], res, find(d) if where is None else where)

    def copy(k, src_dst, slot, source=None, sems=None):
        return pltpu.make_async_remote_copy(
            src_ref=(packed if source is None else source).at[k], dst_ref=arrived.at[slot],
            send_sem=(send_sem if sems is None else sems).at[k], recv_sem=recv_sem.at[slot],
            device_id={"col": src_dst}, device_id_type=pl.DeviceIdType.MESH,
        )

    def send_band(place):
        def one(j):
            pack(place * quarter + j, target(place, j))

            @pl.when(j > 0)
            def _():
                copy(place * quarter + j - 1, target(place, j - 1), me).start()

        if place != OWN:
            if quarter <= 16:
                for j in range(quarter):
                    pack(place * quarter + j, target(place, j), None if place else early[j])
                    if j:
                        copy(place * quarter + j - 1, target(place, j - 1), me).start()
            else:
                loop(0, quarter, one)
            copy((place + 1) * quarter - 1, target(place, quarter - 1), me).start()
        else:
            def local(j):
                pack(place * quarter + j, target(place, j))

            loop(0, quarter, local)

            def send(j):
                copy(place * quarter + j, target(place, j), me).start()

            loop(1, quarter, send)

    def tell(semaphore, d):
        pl.semaphore_signal(
            semaphore, inc=1, device_id={"col": d}, device_id_type=pl.DeviceIdType.MESH)

    for q in range(BANDS):
        @pl.when(band == q)
        def _(q=q):
            pl.semaphore_wait(barrier, (2 * quarter - 1, 3 * quarter - 1, half, n - 1)[q])
            if q == 1:
                tell(near, me - quarter)
                tell(near, me + quarter)
            if q == 3:
                for away in range(1, BANDS):
                    if not (relayed and away == 2):
                        tell(far, me - away * quarter)

    def spread(t, rows):
        wide[:, pl.ds(t, 1), :] = rows.astype(jnp.float32)[:, None, :]

    def burst(count, pack_one, copy_one):
        for i in range(count):
            pack_one(i)
            if i:
                copy_one(i - 1).start()
        copy_one(count - 1).start()

    def own_band(first):
        peer = [band * quarter + (seat + j) % quarter for j in range(quarter)]
        for j in range(quarter):
            pack(first + j, peer[j])
        for j in range(1, quarter):
            copy(first + j, peer[j], me).start()

    def send_to(first, dest):
        burst(quarter, lambda j: pack(first + j, dest * quarter + j),
              lambda j: copy(first + j, dest * quarter + j, me))

    def take_from(src):
        copy(0, src, src).wait_recv()
        spread(src, arrived[src])

    def take_own():
        for j in range(1, quarter):
            take_from(band * quarter + (seat + j) % quarter)

    def sent(k, source=None, sems=None):
        copy(k, me, me, source, sems).wait_send()

    if relayed:
        tail = -(-(blocks - MOST * (groups - 1)) * PLEV // TILE) * TILE
        mirror = jnp.where(band == 1, me + quarter, me - quarter)

        def stage_copies(t):
            first, last = STAGES[t], min(STAGES[t + 1], groups)
            spans = [pl.ds(first, last - first)] if last < groups else [
                pl.ds(first, last - 1 - first), (groups - 1, pl.ds(0, tail))]
            return [
                pltpu.make_async_remote_copy(
                    src_ref=queued.at[span], dst_ref=lists[t].at[span],
                    send_sem=queue_sem.at[2 * t + i], recv_sem=queue_sem.at[2 * STEPS + 2 * t + i],
                    device_id={"col": mirror}, device_id_type=pl.DeviceIdType.MESH)
                for i, span in enumerate(spans)
            ]

        def local(j):
            return copy(j, quarter + j, me)

        @pl.when(band == 0)
        def _():
            for j in range(quarter):
                pack(j, quarter + j)
                if 0 < j <= EARLY:
                    local(j - 1).start()

        @pl.when(band == 3)
        def _():
            send_to(0, EDGE[1][0])

        @pl.when(inner)
        def _():
            for g in range(groups):
                fill(queued.at[g], res, queue[MOST * g:MOST * g + MOST],
                     ROWS if g < groups - 1 else tail)
                for t in range(STEPS - 1):
                    if g == STAGES[t + 1]:
                        for c in stage_copies(t):
                            c.start()
            for c in stage_copies(STEPS - 1):
                c.start()

            @pl.when(band == 2)
            def _():
                pl.semaphore_wait(near, 1)
                pl.semaphore_wait(far, 1)

            send_to(0, jnp.where(band == 1, 0, 3))

        own_band(OWN_AT * quarter)
        spread(me, packed[OWN_AT * quarter])

        def take_edge(place, j):
            take_from(jnp.where(band == 0, EDGE_TAKE[0][place], EDGE_TAKE[1][place]) * quarter + j)

        @pl.when(band == 0)
        def _():
            pl.semaphore_wait(near, 1)
            pl.semaphore_wait(far, 1)
            for j in range(EARLY, quarter):
                local(j).start()

        @pl.when(jnp.logical_not(inner))
        def _():
            cross = [jnp.where(band == 0, p * quarter + a, q * quarter + b)
                     for (p, a), (q, b) in zip(*[
                         [(p, a * quarter // 4 + i) for p, a in order for i in range(quarter // 4)]
                         for order in CROSS])]
            burst(half, lambda i: pack(half + i, cross[i]), lambda i: copy(half + i, cross[i], me))
            take_own()

            for place in range(1, BANDS):
                for j in range(quarter):
                    take_edge(place, j)
            for k in range(2 * quarter, 4 * quarter):
                sent(k)

        @pl.when(inner)
        def _():
            outer = jnp.where(band == 1, 0, 3)
            peers = [outer * quarter + j for j in range(quarter)]
            peers += [band * quarter + (seat + j) % quarter for j in range(1, quarter)]
            peers += [me]
            where = [locate(d) for d in peers]
            def pass_on(i):
                return copy(i, peers[i], mirror, again, again_sem)

            for t in range(STEPS):
                for c in stage_copies(t):
                    c.wait_recv()
                for g in range(STAGES[t]):
                    lists[t][g] = lists[t - 1][g]
                if t < STEPS - 1:
                    @pl.when(band == 1)
                    def _(t=t):
                        for i in range(STAGES[t], STAGES[t + 1]):
                            fill(again.at[i], lists[t], [
                                jnp.where(w == groups, STAGES[t + 1], w) for w in where[i]])
                        for i in range(STAGES[t], STAGES[t + 1]):
                            pass_on(i).start()

            @pl.when(band == 2)
            def _():
                for i in range(STAGES[STEPS - 1]):
                    fill(again.at[i], lists[STEPS - 1], where[i])
                    if i:
                        pass_on(i - 1).start()
                pass_on(STAGES[STEPS - 1] - 1).start()

            for i in range(STAGES[STEPS - 1], half):
                fill(again.at[i], lists[STEPS - 1], where[i])
                if i > STAGES[STEPS - 1]:
                    pass_on(i - 1).start()
            take_own()
            for j in range(quarter):
                take_from(outer * quarter + j)
            spread(mirror, again[half - 1])
            for j in range(1, quarter):
                take_from((BANDS - 1 - band) * quarter + (seat + j) % quarter)
            for j in range(quarter):
                take_from((BANDS - 1 - outer) * quarter + j)
            for t in range(STEPS):
                for c in stage_copies(t):
                    c.wait_send()
            for i in range(half - 1):
                sent(i, again, again_sem)

        for k in range(quarter):
            sent(k)
        for k in range(OWN_AT * quarter + 1, (OWN_AT + 1) * quarter):
            sent(k)
    else:
        send_band(0)

        @pl.when(band == 0)
        def _():
            pl.semaphore_wait(near, 1)

        send_band(1)

        @pl.when(band == 2)
        def _():
            pl.semaphore_wait(near, 1)

        send_band(2)

        @pl.when(band < 3)
        def _():
            pl.semaphore_wait(far, 1)

        send_band(3)

        spread(me, packed[OWN * quarter])

        def take(place):
            def one(j):
                src = choose(TAKE, place, band) * quarter + ((seat + quarter - j) % quarter if place == 0 else j)
                copy(0, src, src).wait_recv()
                spread(src, arrived[src])

            loop(1 if place == 0 else 0, quarter, one)

        for place in range(BANDS):
            take(place)

        loop(0, OWN * quarter, sent)
        loop(OWN * quarter + 1, n, sent)

    turn = before(me)
    turn = turn - MOST * third(turn)
    for s in range(MOST):
        series[s] = wide[pl.ds(shift(s, turn) * PLEV, PLEV)].astype(jnp.bfloat16)


def close(tm, series, tm_out, series_out, sems):
    first = pltpu.make_async_copy(series, series_out, sems.at[0])
    second = pltpu.make_async_copy(tm, tm_out, sems.at[1])
    first.start()
    second.start()
    first.wait()
    second.wait()


def per_device(fields, level_count, owner, band_start, interp_weights):
    n = lax.axis_size("col")
    blocks = owner.shape[0]
    anywhere = pl.BlockSpec(memory_space=pl.ANY)
    cols = blocks * CBLK
    vmem = pl.BlockSpec(memory_space=pltpu.VMEM)
    grant = 2 * cols * TALL + 2 * CBLK * ROWS * (blocks + 1 + 2 * n) + 4 * CBLK * n * ROWS
    grant += blocks * CBLK * 4 * 16 + 2 * cols * 48 + 2 * n * ROWS * CBLK + blocks * WIDE * 512 + (3 << 20)
    grant += 2 * (blocks + n) * ROWS * CBLK
    timemajor, series = pl.pallas_call(
        functools.partial(kernel, n, blocks),
        out_shape=(
            jax.ShapeDtypeStruct((1, PLEV, cols), jnp.bfloat16),
            jax.ShapeDtypeStruct((MOST, PLEV, n, CBLK), jnp.bfloat16),
        ),
        in_specs=[pl.BlockSpec(memory_space=pltpu.HBM)] * 5,
        out_specs=(vmem, vmem),
        scratch_shapes=[
            pltpu.VMEM((LEV, cols), jnp.bfloat16),
            pltpu.VMEM((blocks, CBLK), jnp.int32),
            pltpu.SMEM((blocks,), jnp.int32),
            pltpu.VMEM((blocks, PLEV), jnp.int32),
            pltpu.VMEM((blocks * BAND, PLEV), jnp.float32),
            pltpu.VMEM((blocks, CBLK), jnp.float32),
            pltpu.VMEM((blocks * BAND, CBLK), jnp.float32),
            pltpu.VMEM((blocks, WIDE, LEV), jnp.bfloat16),
            pltpu.VMEM((blocks + 1, ROWS, CBLK), jnp.bfloat16),
            pltpu.VMEM((n, ROWS, CBLK), jnp.bfloat16),
            pltpu.VMEM((n, ROWS, CBLK), jnp.bfloat16),
            pltpu.VMEM((ROWS, n, CBLK), jnp.float32),
            pltpu.SemaphoreType.DMA((len(CUTS) - 1,)),
            pltpu.SemaphoreType.DMA((4,)),
            pltpu.SemaphoreType.DMA((n,)),
            pltpu.SemaphoreType.DMA((n,)),
            pltpu.SemaphoreType.REGULAR,
            pltpu.SemaphoreType.REGULAR,
            pltpu.VMEM((-(-blocks // MOST), ROWS, CBLK), jnp.bfloat16),
            pltpu.VMEM((n // 2, ROWS, CBLK), jnp.bfloat16),
            pltpu.SemaphoreType.DMA((4 * STEPS,)),
            pltpu.SemaphoreType.DMA((n // 2,)),
            *[pltpu.VMEM((min(last, -(-blocks // MOST)) + 1, ROWS, CBLK), jnp.bfloat16) for last in STAGES[1:]],
        ],
        compiler_params=pltpu.CompilerParams(
            collective_id=0, has_side_effects=True, vmem_limit_bytes=grant
        ),
    )(
        *[pltpu.with_memory_space_constraint(x, pltpu.HBM) for x in (
            fields, level_count.reshape(blocks, CBLK), owner, band_start,
            jnp.swapaxes(interp_weights, 1, 2).reshape(blocks * BAND, PLEV),
        )]
    )
    return pl.pallas_call(
        close,
        out_shape=(
            jax.ShapeDtypeStruct((1, PLEV, cols), jnp.bfloat16),
            jax.ShapeDtypeStruct((MOST, PLEV, n, CBLK), jnp.bfloat16),
        ),
        in_specs=[vmem, vmem],
        out_specs=(anywhere, anywhere),
        scratch_shapes=[pltpu.SemaphoreType.DMA((2,))],
        compiler_params=pltpu.CompilerParams(vmem_limit_bytes=3 << 20),
    )(timemajor, series)


def solution(mesh):
    placed = (P(("groups", "col"), None, None), P(), P(), P(), P())
    return jax.shard_map(
        per_device,
        mesh=mesh,
        in_specs=placed,
        out_specs=(P(("groups", "col"), None, None), P(("groups", "col"), None, None, None)),
        check_vma=False,
    )
```

```python
import functools

import jax
import jax.numpy as jnp
from jax import lax
from jax.experimental import pallas as pl
from jax.experimental.pallas import tpu as pltpu
from jax.sharding import PartitionSpec as P

LEV = 137
PLEV = 37
BAND = 4
CBLK = 128
MOST = 3
TILE = 16
LOW = (LEV // 2 - 1) // TILE * TILE
TALL = -(-LEV // TILE) * TILE
ROWS = -(-MOST * PLEV // TILE) * TILE
WIDE = -(-PLEV // TILE) * TILE
BANDS = 4
CUTS = (0, 16)
SEND = ((1, 2, 0, 3), (2, 0, 1, 3), (0, 1, 2, 3), (0, 2, 3, 1))
OWN = 2
TAKE = ((0, 3, 2, 1), (1, 0, 3, 2), (2, 3, 0, 1), (3, 2, 0, 1))
OWN_AT = 1
EARLY = (4, 3)
CROSS = (((3, 0), (3, 1), (3, 2), (3, 3), (2, 0), (2, 1), (2, 2), (2, 3)),
         ((2, 0), (2, 1), (2, 2), (0, 0), (2, 3), (0, 1), (0, 2), (1, 0), (0, 3), (1, 1), (1, 2), (1, 3)))
EDGE_TAKE = ((0, 1, 3, 2), (3, 2, 0, 1))
STAGES = (0, 2, 4, 1 << 20)
STEPS = len(STAGES) - 1


def loop(first, last, body):
    if last - first <= 16:
        for i in range(first, last):
            body(i)
    else:

        def step(i, carry):
            body(i)
            return carry

        lax.fori_loop(first, last, step, 0)


def choose(table, place, band):
    value = jnp.int32(table[0][place])
    for q in range(1, BANDS):
        value = jnp.where(band == q, jnp.int32(table[q][place]), value)
    return value


def kernel(n, blocks, fields, counts_in, owner_in, starts_in, weights_in, tm, series,
           data, counts, owner, starts, weights, start_row, weight_row, matrix, res, packed, arrived, wide,
           load_sem, small_sem, send_sem, recv_sem, near, far, queued, again, queue_sem, again_sem, line, *lists):
    me = lax.axis_index("col")
    half = n // 2
    quarter = n // BANDS
    band = me // quarter
    seat = me % quarter
    barrier = pltpu.get_barrier_semaphore()

    smalls = []
    for i, (src, dst) in enumerate(
        [(owner_in, owner), (starts_in, starts), (weights_in, weights), (counts_in, counts)]
    ):
        small = pltpu.make_async_copy(src, dst, small_sem.at[i])
        small.start()
        smalls.append(small)
    loads = []
    for i, (first, last) in enumerate(zip(CUTS, CUTS[1:])):
        span = pl.ds(blocks * first // 16 * CBLK, blocks * (last - first) // 16 * CBLK)
        load = pltpu.make_async_copy(fields.at[0, :, span], data.at[:, span], load_sem.at[i])
        load.start()
        loads.append(load)

    relayed = blocks <= 16 and quarter <= 16

    def greet(d):
        pl.semaphore_signal(
            barrier, inc=1, device_id={"col": d}, device_id_type=pl.DeviceIdType.MESH)

    @pl.when(band < 2)
    def _():
        loop(1, n, lambda i: greet((me + i) % n))

    @pl.when(band == 2)
    def _():
        if relayed:
            loop(0, quarter // 2, lambda i: greet(quarter + seat // (quarter // 2) * (quarter // 2) + i))
        else:
            loop(0, quarter, lambda i: greet(quarter + i))
        loop(0, quarter, lambda i: greet(half + quarter + i))

    @pl.when(band == 3)
    def _():
        loop(1, quarter, lambda i: greet(half + quarter + (seat + i) % quarter))

    res[blocks] = jnp.zeros(res.shape[1:], jnp.bfloat16)
    for part in lists:
        part[part.shape[0] - 1] = jnp.zeros(part.shape[1:], jnp.bfloat16)
    for small in smalls[:-1]:
        small.wait()

    start_row[...] = jnp.concatenate(
        [starts[...].astype(jnp.float32),
         jnp.full((blocks, CBLK - PLEV), -float(CBLK), jnp.float32)], axis=1)
    weight_row[...] = jnp.concatenate(
        [weights[...], jnp.zeros((blocks * BAND, CBLK - PLEV), jnp.float32)], axis=1)

    unit = 1 << blocks.bit_length()
    groups = -(-blocks // MOST)

    def third(x):
        return (x * 43) >> 7

    def shift(c, turn):
        return jnp.where(c + turn >= MOST, c + turn - MOST, c + turn)

    base = (1 - me // half) * half

    def away(d):
        return jnp.where(d < base, d - base + n, d - base)

    if relayed:
        keys = [away(owner[b]) * unit + b for b in range(blocks)]
        before = jnp.int32(0)
        for key in keys:
            before = before + jnp.where(key < half * unit, 1, 0)
        size = 1 << (blocks - 1).bit_length()
        ranked = keys + [jnp.int32(n * unit + blocks)] * (size - blocks)
        p = 1
        while p < size:
            k = p
            while k >= 1:
                for j in range(k % p, size - k, 2 * k):
                    for i in range(min(k, size - j - k)):
                        if (i + j) // (2 * p) == (i + j + k) // (2 * p):
                            x, y = ranked[i + j], ranked[i + j + k]
                            ranked[i + j], ranked[i + j + k] = jnp.minimum(x, y), jnp.maximum(x, y)
                k //= 2
            p *= 2
        ranked = ranked[:blocks]
        for i in range(blocks):
            line[i] = ranked[i]
        for i in range(MOST):
            line[blocks + i] = jnp.int32(n * unit + blocks)
        queue = [key & (unit - 1) for key in ranked] + [jnp.int32(blocks)] * (groups * MOST - blocks)

    def places(d):
        first = jnp.int32(0)
        for key in keys:
            first = first + jnp.where(key < away(d) * unit, 1, 0)
        listed = first - jnp.where(away(d) >= half, before, 0)
        return first, listed, listed - MOST * third(listed)

    def parts(d):
        first, listed, turn = places(d)
        for c in range(MOST):
            step = jnp.where(c >= turn, c - turn, c - turn + MOST)
            key = line[first + step]
            yield key < (away(d) + 1) * unit, key & (unit - 1), listed + step

    def find(d):
        if relayed:
            return [jnp.where(mine, block, blocks) for mine, block, place in parts(d)]

        def look(i, found):
            b = blocks - 1 - i
            return jnp.where(owner[b] == d, found * unit + b, found)

        found = jnp.int32(blocks)
        for s in range(1, MOST):
            found = found * unit + blocks
        if blocks <= 16:
            for i in range(blocks):
                found = look(i, found)
        else:
            found = lax.fori_loop(0, blocks, look, found)
        return [(found // unit ** s) % unit for s in range(MOST)]

    def locate(d):
        return [jnp.where(mine, third(place), groups) for mine, block, place in parts(d)]

    def target(place, j):
        return choose(SEND, place, band) * quarter + ((seat + j) % quarter if place == OWN else j)

    early = None
    if relayed:
        inner = (band == 1) | (band == 2)
    elif quarter <= 16:
        early = [find(target(0, j)) for j in range(quarter)]

    row = lax.broadcasted_iota(jnp.int32, (TILE, CBLK), 0).astype(jnp.float32).astype(jnp.bfloat16)
    zero = jnp.zeros((TILE, CBLK), jnp.bfloat16)

    def packed_row(ref, i):
        return jnp.broadcast_to(ref[pl.ds(i, 1), :], (TILE, CBLK)).astype(jnp.bfloat16)

    def build(b):
        first = packed_row(start_row, b)
        terms = [packed_row(weight_row, b * BAND + k) for k in range(BAND)]
        parts = []
        for i in range(0, TALL, TILE):
            offset = (row + float(i)) - first
            part = zero
            for k in range(BAND):
                part = jnp.where(offset == float(k), terms[k], part)
            parts.append(part)
        matrix[b] = jnp.concatenate(parts, axis=0).T[:WIDE, :LEV]

    loop(0, blocks, build)

    def interpolate(b):
        cols = pl.ds(pl.multiple_of(b * CBLK, CBLK), CBLK)
        count = jnp.broadcast_to(
            counts[pl.ds(b, 1), :].astype(jnp.float32), (TILE, CBLK)).astype(jnp.bfloat16)
        filled = [data[:LOW, cols]]
        last = zero
        ends = 0.0
        for i in range(LOW, LEV, TILE):
            size = min(TILE, LEV - i)
            part = jnp.where(row[:size] + float(i + 1) == count[:size], data[i:i + size, cols], zero[:size])
            if size == TILE:
                last = last + part
            else:
                ends = jnp.sum(part.astype(jnp.float32), axis=0, keepdims=True)
        last = jnp.sum(last.astype(jnp.float32), axis=0, keepdims=True) + ends
        last = jnp.broadcast_to(last, (TILE, CBLK)).astype(jnp.bfloat16)
        for i in range(LOW, LEV, TILE):
            size = min(TILE, LEV - i)
            filled.append(jnp.where(row[:size] + float(i) < count[:size], data[i:i + size, cols], last[:size]))
        out = jnp.dot(
            matrix[b], jnp.concatenate(filled, axis=0), preferred_element_type=jnp.float32)[:PLEV]
        tm[0, :, cols] = out.astype(jnp.bfloat16)
        res[b] = jnp.concatenate(
            [out] * MOST + [jnp.zeros((ROWS - MOST * PLEV, CBLK), jnp.float32)], axis=0,
        ).astype(jnp.bfloat16)

    for small in smalls[-1:]:
        small.wait()
    for load, first, last in zip(loads, CUTS, CUTS[1:]):
        load.wait()
        loop(blocks * first // 16, blocks * last // 16, interpolate)

    def fill(target, source, where, rows=ROWS):
        for i in range(0, rows, TILE):
            slots = [s for s in range(MOST) if s * PLEV < i + TILE and (s + 1) * PLEV > i]
            part = source[where[slots[0]], pl.ds(i, TILE)]
            for s in slots[1:]:
                part = jnp.where(
                    row < float(s * PLEV - i), part, source[where[s], pl.ds(i, TILE)])
            target[pl.ds(i, TILE)] = part

    def pack(k, d, where=None):
        fill(packed.at[k], res, find(d) if where is None else where)

    def copy(k, src_dst, slot, source=None, sems=None):
        return pltpu.make_async_remote_copy(
            src_ref=(packed if source is None else source).at[k], dst_ref=arrived.at[slot],
            send_sem=(send_sem if sems is None else sems).at[k], recv_sem=recv_sem.at[slot],
            device_id={"col": src_dst}, device_id_type=pl.DeviceIdType.MESH,
        )

    def send_band(place):
        def one(j):
            pack(place * quarter + j, target(place, j))

            @pl.when(j > 0)
            def _():
                copy(place * quarter + j - 1, target(place, j - 1), me).start()

        if place != OWN:
            if quarter <= 16:
                for j in range(quarter):
                    pack(place * quarter + j, target(place, j), None if place else early[j])
                    if j:
                        copy(place * quarter + j - 1, target(place, j - 1), me).start()
            else:
                loop(0, quarter, one)
            copy((place + 1) * quarter - 1, target(place, quarter - 1), me).start()
        else:
            def local(j):
                pack(place * quarter + j, target(place, j))

            loop(0, quarter, local)

            def send(j):
                copy(place * quarter + j, target(place, j), me).start()

            loop(1, quarter, send)

    def tell(semaphore, d):
        pl.semaphore_signal(
            semaphore, inc=1, device_id={"col": d}, device_id_type=pl.DeviceIdType.MESH)

    for q in range(BANDS):
        @pl.when(band == q)
        def _(q=q):
            pl.semaphore_wait(barrier, (
                2 * quarter - 1, 2 * quarter - 1 + (quarter // 2 if relayed else quarter), half, n - 1)[q])
            if q == 1:
                tell(near, me - quarter)
                if relayed:
                    tell(near, (seat + quarter // 2) % quarter)
                else:
                    tell(near, me + quarter)
            if q == 3:
                for away in range(1, BANDS):
                    if not (relayed and away == 2):
                        tell(far, me - away * quarter)

    def spread(t, rows):
        wide[:, pl.ds(t, 1), :] = rows.astype(jnp.float32)[:, None, :]

    def burst(count, pack_one, copy_one):
        for i in range(count):
            pack_one(i)
            if i:
                copy_one(i - 1).start()
        copy_one(count - 1).start()

    def own_band(first):
        peer = [band * quarter + (seat + j) % quarter for j in range(quarter)]
        for j in range(quarter):
            pack(first + j, peer[j])
        for j in range(1, quarter):
            copy(first + j, peer[j], me).start()

    def send_to(first, dest):
        burst(quarter, lambda j: pack(first + j, dest * quarter + j),
              lambda j: copy(first + j, dest * quarter + j, me))

    def take_from(src):
        copy(0, src, src).wait_recv()
        spread(src, arrived[src])

    def take_own():
        for j in range(1, quarter):
            take_from(band * quarter + (seat + j) % quarter)

    def sent(k, source=None, sems=None):
        copy(k, me, me, source, sems).wait_send()

    if relayed:
        tail = -(-(blocks - MOST * (groups - 1)) * PLEV // TILE) * TILE
        mirror = jnp.where(band == 1, me + quarter, me - quarter)

        def stage_copies(t):
            first, last = STAGES[t], min(STAGES[t + 1], groups)
            spans = [pl.ds(first, last - first)] if last < groups else [
                pl.ds(first, last - 1 - first), (groups - 1, pl.ds(0, tail))]
            return [
                pltpu.make_async_remote_copy(
                    src_ref=queued.at[span], dst_ref=lists[t].at[span],
                    send_sem=queue_sem.at[2 * t + i], recv_sem=queue_sem.at[2 * STEPS + 2 * t + i],
                    device_id={"col": mirror}, device_id_type=pl.DeviceIdType.MESH)
                for i, span in enumerate(spans)
            ]

        def local(j):
            return copy(j, quarter + j, me)

        @pl.when(band == 0)
        def _():
            for j in range(quarter):
                pack(j, quarter + j)
                if 0 < j <= EARLY[1]:
                    local(j - 1).start()

            @pl.when(seat < quarter // 2)
            def _():
                for j in range(EARLY[1], EARLY[0]):
                    local(j).start()

        def slot_of(i):
            return i if i < quarter else i + quarter

        def spell(order):
            return [p * quarter + a * quarter // 4 + i for p, a in order for i in range(quarter // 4)]

        @pl.when(band == 3)
        def _():
            dests = spell(CROSS[1])
            burst(len(dests), lambda i: pack(slot_of(i), dests[i]), lambda i: copy(slot_of(i), dests[i], me))

        @pl.when(inner)
        def _():
            for g in range(groups):
                fill(queued.at[g], res, queue[MOST * g:MOST * g + MOST],
                     ROWS if g < groups - 1 else tail)
                for t in range(STEPS - 1):
                    if g == STAGES[t + 1]:
                        for c in stage_copies(t):
                            c.start()
            for c in stage_copies(STEPS - 1):
                c.start()

            @pl.when(band == 2)
            def _():
                pl.semaphore_wait(far, 1)

            send_to(0, jnp.where(band == 1, 0, 3))

        own_band(OWN_AT * quarter)
        spread(me, packed[OWN_AT * quarter])

        def take_edge(place, j):
            take_from(jnp.where(band == 0, EDGE_TAKE[0][place], EDGE_TAKE[1][place]) * quarter + j)

        @pl.when(band == 0)
        def _():
            pl.semaphore_wait(near, 2)
            pl.semaphore_wait(far, 1)

            @pl.when(seat >= quarter // 2)
            def _():
                for j in range(EARLY[1], EARLY[0]):
                    local(j).start()

            for j in range(EARLY[0], quarter):
                local(j).start()
            dests = spell(CROSS[0])
            burst(half, lambda i: pack(half + i, dests[i]), lambda i: copy(half + i, dests[i], me))

        @pl.when(jnp.logical_not(inner))
        def _():
            take_own()

            for place in range(1, BANDS):
                for j in range(quarter):
                    take_edge(place, j)
            for k in range(2 * quarter, 4 * quarter):
                sent(k)

        @pl.when(inner)
        def _():
            outer = jnp.where(band == 1, 0, 3)
            peers = [outer * quarter + j for j in range(quarter)]
            peers += [band * quarter + (seat + j) % quarter for j in range(1, quarter)]
            peers += [me]
            where = [locate(d) for d in peers]
            def pass_on(i):
                return copy(i, peers[i], mirror, again, again_sem)

            for t in range(STEPS):
                for c in stage_copies(t):
                    c.wait_recv()
                for g in range(STAGES[t]):
                    lists[t][g] = lists[t - 1][g]
                if t < STEPS - 1:
                    @pl.when(band == 1)
                    def _(t=t):
                        for i in range(STAGES[t], STAGES[t + 1]):
                            fill(again.at[i], lists[t], [
                                jnp.where(w == groups, STAGES[t + 1], w) for w in where[i]])
                        for i in range(STAGES[t], STAGES[t + 1]):
                            pass_on(i).start()

            @pl.when(band == 2)
            def _():
                for i in range(STAGES[STEPS - 1]):
                    fill(again.at[i], lists[STEPS - 1], where[i])
                    if i:
                        pass_on(i - 1).start()
                pass_on(STAGES[STEPS - 1] - 1).start()

            for i in range(STAGES[STEPS - 1], half):
                fill(again.at[i], lists[STEPS - 1], where[i])
                if i > STAGES[STEPS - 1]:
                    pass_on(i - 1).start()
            take_own()
            for j in range(quarter):
                take_from(outer * quarter + j)
            spread(mirror, again[half - 1])
            for j in range(1, quarter):
                take_from((BANDS - 1 - band) * quarter + (seat + j) % quarter)
            for j in range(quarter):
                take_from((BANDS - 1 - outer) * quarter + j)
            for t in range(STEPS):
                for c in stage_copies(t):
                    c.wait_send()
            for i in range(half - 1):
                sent(i, again, again_sem)

        for k in range(quarter):
            sent(k)
        for k in range(OWN_AT * quarter + 1, (OWN_AT + 1) * quarter):
            sent(k)
    else:
        send_band(0)

        @pl.when(band == 0)
        def _():
            pl.semaphore_wait(near, 1)

        send_band(1)

        @pl.when(band == 2)
        def _():
            pl.semaphore_wait(near, 1)

        send_band(2)

        @pl.when(band < 3)
        def _():
            pl.semaphore_wait(far, 1)

        send_band(3)

        spread(me, packed[OWN * quarter])

        def take(place):
            def one(j):
                src = choose(TAKE, place, band) * quarter + ((seat + quarter - j) % quarter if place == 0 else j)
                copy(0, src, src).wait_recv()
                spread(src, arrived[src])

            loop(1 if place == 0 else 0, quarter, one)

        for place in range(BANDS):
            take(place)

        loop(0, OWN * quarter, sent)
        loop(OWN * quarter + 1, n, sent)

    turn = places(me)[2] if relayed else jnp.int32(0)
    for s in range(MOST):
        series[s] = wide[pl.ds(shift(s, turn) * PLEV, PLEV)].astype(jnp.bfloat16)


def close(tm, series, tm_out, series_out, sems):
    first = pltpu.make_async_copy(series, series_out, sems.at[0])
    second = pltpu.make_async_copy(tm, tm_out, sems.at[1])
    first.start()
    second.start()
    first.wait()
    second.wait()


def per_device(fields, level_count, owner, band_start, interp_weights):
    n = lax.axis_size("col")
    blocks = owner.shape[0]
    anywhere = pl.BlockSpec(memory_space=pl.ANY)
    cols = blocks * CBLK
    vmem = pl.BlockSpec(memory_space=pltpu.VMEM)
    grant = 2 * cols * TALL + 2 * CBLK * ROWS * (blocks + 1 + 2 * n) + 4 * CBLK * n * ROWS
    grant += blocks * CBLK * 4 * 16 + 2 * cols * 48 + 2 * n * ROWS * CBLK + blocks * WIDE * 512 + (3 << 20)
    grant += 2 * (blocks + n) * ROWS * CBLK
    timemajor, series = pl.pallas_call(
        functools.partial(kernel, n, blocks),
        out_shape=(
            jax.ShapeDtypeStruct((1, PLEV, cols), jnp.bfloat16),
            jax.ShapeDtypeStruct((MOST, PLEV, n, CBLK), jnp.bfloat16),
        ),
        in_specs=[pl.BlockSpec(memory_space=pltpu.HBM)] * 5,
        out_specs=(vmem, vmem),
        scratch_shapes=[
            pltpu.VMEM((LEV, cols), jnp.bfloat16),
            pltpu.VMEM((blocks, CBLK), jnp.int32),
            pltpu.SMEM((blocks,), jnp.int32),
            pltpu.VMEM((blocks, PLEV), jnp.int32),
            pltpu.VMEM((blocks * BAND, PLEV), jnp.float32),
            pltpu.VMEM((blocks, CBLK), jnp.float32),
            pltpu.VMEM((blocks * BAND, CBLK), jnp.float32),
            pltpu.VMEM((blocks, WIDE, LEV), jnp.bfloat16),
            pltpu.VMEM((blocks + 1, ROWS, CBLK), jnp.bfloat16),
            pltpu.VMEM((n, ROWS, CBLK), jnp.bfloat16),
            pltpu.VMEM((n, ROWS, CBLK), jnp.bfloat16),
            pltpu.VMEM((ROWS, n, CBLK), jnp.float32),
            pltpu.SemaphoreType.DMA((len(CUTS) - 1,)),
            pltpu.SemaphoreType.DMA((4,)),
            pltpu.SemaphoreType.DMA((n,)),
            pltpu.SemaphoreType.DMA((n,)),
            pltpu.SemaphoreType.REGULAR,
            pltpu.SemaphoreType.REGULAR,
            pltpu.VMEM((-(-blocks // MOST), ROWS, CBLK), jnp.bfloat16),
            pltpu.VMEM((n // 2, ROWS, CBLK), jnp.bfloat16),
            pltpu.SemaphoreType.DMA((4 * STEPS,)),
            pltpu.SemaphoreType.DMA((n // 2,)),
            pltpu.SMEM((blocks + MOST,), jnp.int32),
            *[pltpu.VMEM((min(last, -(-blocks // MOST)) + 1, ROWS, CBLK), jnp.bfloat16) for last in STAGES[1:]],
        ],
        compiler_params=pltpu.CompilerParams(
            collective_id=0, has_side_effects=True, vmem_limit_bytes=grant
        ),
    )(
        *[pltpu.with_memory_space_constraint(x, pltpu.HBM) for x in (
            fields, level_count.reshape(blocks, CBLK), owner, band_start,
            jnp.swapaxes(interp_weights, 1, 2).reshape(blocks * BAND, PLEV),
        )]
    )
    return pl.pallas_call(
        close,
        out_shape=(
            jax.ShapeDtypeStruct((1, PLEV, cols), jnp.bfloat16),
            jax.ShapeDtypeStruct((MOST, PLEV, n, CBLK), jnp.bfloat16),
        ),
        in_specs=[vmem, vmem],
        out_specs=(anywhere, anywhere),
        scratch_shapes=[pltpu.SemaphoreType.DMA((2,))],
        compiler_params=pltpu.CompilerParams(vmem_limit_bytes=3 << 20),
    )(timemajor, series)


def solution(mesh):
    placed = (P(("groups", "col"), None, None), P(), P(), P(), P())
    return jax.shard_map(
        per_device,
        mesh=mesh,
        in_specs=placed,
        out_specs=(P(("groups", "col"), None, None), P(("groups", "col"), None, None, None)),
        check_vma=False,
    )
```

```python
import functools

import jax
import jax.numpy as jnp
from jax import lax
from jax.experimental import pallas as pl
from jax.experimental.pallas import tpu as pltpu
from jax.sharding import PartitionSpec as P

LEV = 137
PLEV = 37
BAND = 4
CBLK = 128
MOST = 3
TILE = 16
LOW = (LEV // 2 - 1) // TILE * TILE
TALL = -(-LEV // TILE) * TILE
ROWS = -(-MOST * PLEV // TILE) * TILE
WIDE = -(-PLEV // TILE) * TILE
BANDS = 4
CUTS = (0, 16)
SEND = ((1, 2, 0, 3), (2, 0, 1, 3), (0, 1, 2, 3), (0, 2, 3, 1))
OWN = 2
TAKE = ((0, 3, 2, 1), (1, 0, 3, 2), (2, 3, 0, 1), (3, 2, 0, 1))
OWN_AT = 1
EARLY = (4, 3)
CROSS = (((3, 0), (3, 1), (3, 2), (3, 3), (2, 0), (2, 1), (2, 2), (2, 3)),
         ((2, 0), (2, 1), (2, 2), (2, 3), (0, 0), (0, 1), (1, 0), (0, 2), (0, 3), (1, 1), (1, 2), (1, 3)))
EDGE_TAKE = ((0, 1, 3, 2), (3, 2, 0, 1))
STAGES = (0, 2, 4, 1 << 20)
STEPS = len(STAGES) - 1


def loop(first, last, body):
    if last - first <= 16:
        for i in range(first, last):
            body(i)
    else:

        def step(i, carry):
            body(i)
            return carry

        lax.fori_loop(first, last, step, 0)


def choose(table, place, band):
    value = jnp.int32(table[0][place])
    for q in range(1, BANDS):
        value = jnp.where(band == q, jnp.int32(table[q][place]), value)
    return value


def kernel(n, blocks, fields, counts_in, owner_in, starts_in, weights_in, tm, series,
           data, counts, owner, starts, weights, start_row, weight_row, matrix, res, packed, arrived, wide,
           load_sem, small_sem, send_sem, recv_sem, near, far, queued, again, queue_sem, again_sem, line, *lists):
    me = lax.axis_index("col")
    half = n // 2
    quarter = n // BANDS
    band = me // quarter
    seat = me % quarter
    barrier = pltpu.get_barrier_semaphore()

    smalls = []
    for i, (src, dst) in enumerate(
        [(owner_in, owner), (starts_in, starts), (weights_in, weights), (counts_in, counts)]
    ):
        small = pltpu.make_async_copy(src, dst, small_sem.at[i])
        small.start()
        smalls.append(small)
    loads = []
    for i, (first, last) in enumerate(zip(CUTS, CUTS[1:])):
        span = pl.ds(blocks * first // 16 * CBLK, blocks * (last - first) // 16 * CBLK)
        load = pltpu.make_async_copy(fields.at[0, :, span], data.at[:, span], load_sem.at[i])
        load.start()
        loads.append(load)

    relayed = blocks <= 16 and quarter <= 16

    def greet(d):
        pl.semaphore_signal(
            barrier, inc=1, device_id={"col": d}, device_id_type=pl.DeviceIdType.MESH)

    @pl.when(band < 2)
    def _():
        loop(1, n, lambda i: greet((me + i) % n))

    @pl.when(band == 2)
    def _():
        if relayed:
            loop(0, quarter // 2, lambda i: greet(quarter + seat // (quarter // 2) * (quarter // 2) + i))
        else:
            loop(0, quarter, lambda i: greet(quarter + i))
        loop(0, quarter, lambda i: greet(half + quarter + i))

    @pl.when(band == 3)
    def _():
        if relayed:
            part = seat // (quarter // 2) * (quarter // 2)
            loop(1, quarter // 2, lambda i: greet(half + quarter + part + (seat + i) % (quarter // 2)))
        else:
            loop(1, quarter, lambda i: greet(half + quarter + (seat + i) % quarter))

    res[blocks] = jnp.zeros(res.shape[1:], jnp.bfloat16)
    for part in lists:
        part[part.shape[0] - 1] = jnp.zeros(part.shape[1:], jnp.bfloat16)
    for small in smalls[:-1]:
        small.wait()

    start_row[...] = jnp.concatenate(
        [starts[...].astype(jnp.float32),
         jnp.full((blocks, CBLK - PLEV), -float(CBLK), jnp.float32)], axis=1)
    weight_row[...] = jnp.concatenate(
        [weights[...], jnp.zeros((blocks * BAND, CBLK - PLEV), jnp.float32)], axis=1)

    unit = 1 << blocks.bit_length()
    groups = -(-blocks // MOST)

    def third(x):
        return (x * 43) >> 7

    def shift(c, turn):
        return jnp.where(c + turn >= MOST, c + turn - MOST, c + turn)

    base = (1 - me // half) * half

    def away(d):
        return jnp.where(d < base, d - base + n, d - base)

    if relayed:
        keys = [away(owner[b]) * unit + b for b in range(blocks)]
        before = jnp.int32(0)
        for key in keys:
            before = before + jnp.where(key < half * unit, 1, 0)
        size = 1 << (blocks - 1).bit_length()
        ranked = keys + [jnp.int32(n * unit + blocks)] * (size - blocks)
        p = 1
        while p < size:
            k = p
            while k >= 1:
                for j in range(k % p, size - k, 2 * k):
                    for i in range(min(k, size - j - k)):
                        if (i + j) // (2 * p) == (i + j + k) // (2 * p):
                            x, y = ranked[i + j], ranked[i + j + k]
                            ranked[i + j], ranked[i + j + k] = jnp.minimum(x, y), jnp.maximum(x, y)
                k //= 2
            p *= 2
        ranked = ranked[:blocks]
        for i in range(blocks):
            line[i] = ranked[i]
        for i in range(MOST):
            line[blocks + i] = jnp.int32(n * unit + blocks)
        queue = [key & (unit - 1) for key in ranked] + [jnp.int32(blocks)] * (groups * MOST - blocks)

    def places(d):
        first = jnp.int32(0)
        for key in keys:
            first = first + jnp.where(key < away(d) * unit, 1, 0)
        listed = first - jnp.where(away(d) >= half, before, 0)
        return first, listed, listed - MOST * third(listed)

    def parts(d):
        first, listed, turn = places(d)
        for c in range(MOST):
            step = jnp.where(c >= turn, c - turn, c - turn + MOST)
            key = line[first + step]
            yield key < (away(d) + 1) * unit, key & (unit - 1), listed + step

    def find(d):
        if relayed:
            return [jnp.where(mine, block, blocks) for mine, block, place in parts(d)]

        def look(i, found):
            b = blocks - 1 - i
            return jnp.where(owner[b] == d, found * unit + b, found)

        found = jnp.int32(blocks)
        for s in range(1, MOST):
            found = found * unit + blocks
        if blocks <= 16:
            for i in range(blocks):
                found = look(i, found)
        else:
            found = lax.fori_loop(0, blocks, look, found)
        return [(found // unit ** s) % unit for s in range(MOST)]

    def locate(d):
        return [jnp.where(mine, third(place), groups) for mine, block, place in parts(d)]

    def target(place, j):
        return choose(SEND, place, band) * quarter + ((seat + j) % quarter if place == OWN else j)

    early = None
    if relayed:
        inner = (band == 1) | (band == 2)
    elif quarter <= 16:
        early = [find(target(0, j)) for j in range(quarter)]

    row = lax.broadcasted_iota(jnp.int32, (TILE, CBLK), 0).astype(jnp.float32).astype(jnp.bfloat16)
    zero = jnp.zeros((TILE, CBLK), jnp.bfloat16)

    def packed_row(ref, i):
        return jnp.broadcast_to(ref[pl.ds(i, 1), :], (TILE, CBLK)).astype(jnp.bfloat16)

    def build(b):
        first = packed_row(start_row, b)
        terms = [packed_row(weight_row, b * BAND + k) for k in range(BAND)]
        parts = []
        for i in range(0, TALL, TILE):
            offset = (row + float(i)) - first
            part = zero
            for k in range(BAND):
                part = jnp.where(offset == float(k), terms[k], part)
            parts.append(part)
        matrix[b] = jnp.concatenate(parts, axis=0).T[:WIDE, :LEV]

    loop(0, blocks, build)

    def interpolate(b):
        cols = pl.ds(pl.multiple_of(b * CBLK, CBLK), CBLK)
        count = jnp.broadcast_to(
            counts[pl.ds(b, 1), :].astype(jnp.float32), (TILE, CBLK)).astype(jnp.bfloat16)
        filled = [data[:LOW, cols]]
        last = zero
        ends = 0.0
        for i in range(LOW, LEV, TILE):
            size = min(TILE, LEV - i)
            part = jnp.where(row[:size] + float(i + 1) == count[:size], data[i:i + size, cols], zero[:size])
            if size == TILE:
                last = last + part
            else:
                ends = jnp.sum(part.astype(jnp.float32), axis=0, keepdims=True)
        last = jnp.sum(last.astype(jnp.float32), axis=0, keepdims=True) + ends
        last = jnp.broadcast_to(last, (TILE, CBLK)).astype(jnp.bfloat16)
        for i in range(LOW, LEV, TILE):
            size = min(TILE, LEV - i)
            filled.append(jnp.where(row[:size] + float(i) < count[:size], data[i:i + size, cols], last[:size]))
        out = jnp.dot(
            matrix[b], jnp.concatenate(filled, axis=0), preferred_element_type=jnp.float32)[:PLEV]
        tm[0, :, cols] = out.astype(jnp.bfloat16)
        res[b] = jnp.concatenate(
            [out] * MOST + [jnp.zeros((ROWS - MOST * PLEV, CBLK), jnp.float32)], axis=0,
        ).astype(jnp.bfloat16)

    for small in smalls[-1:]:
        small.wait()
    for load, first, last in zip(loads, CUTS, CUTS[1:]):
        load.wait()
        loop(blocks * first // 16, blocks * last // 16, interpolate)

    def fill(target, source, where, rows=ROWS):
        for i in range(0, rows, TILE):
            slots = [s for s in range(MOST) if s * PLEV < i + TILE and (s + 1) * PLEV > i]
            part = source[where[slots[0]], pl.ds(i, TILE)]
            for s in slots[1:]:
                part = jnp.where(
                    row < float(s * PLEV - i), part, source[where[s], pl.ds(i, TILE)])
            target[pl.ds(i, TILE)] = part

    def pack(k, d, where=None):
        fill(packed.at[k], res, find(d) if where is None else where)

    def copy(k, src_dst, slot, source=None, sems=None):
        return pltpu.make_async_remote_copy(
            src_ref=(packed if source is None else source).at[k], dst_ref=arrived.at[slot],
            send_sem=(send_sem if sems is None else sems).at[k], recv_sem=recv_sem.at[slot],
            device_id={"col": src_dst}, device_id_type=pl.DeviceIdType.MESH,
        )

    def send_band(place):
        def one(j):
            pack(place * quarter + j, target(place, j))

            @pl.when(j > 0)
            def _():
                copy(place * quarter + j - 1, target(place, j - 1), me).start()

        if place != OWN:
            if quarter <= 16:
                for j in range(quarter):
                    pack(place * quarter + j, target(place, j), None if place else early[j])
                    if j:
                        copy(place * quarter + j - 1, target(place, j - 1), me).start()
            else:
                loop(0, quarter, one)
            copy((place + 1) * quarter - 1, target(place, quarter - 1), me).start()
        else:
            def local(j):
                pack(place * quarter + j, target(place, j))

            loop(0, quarter, local)

            def send(j):
                copy(place * quarter + j, target(place, j), me).start()

            loop(1, quarter, send)

    def tell(semaphore, d):
        pl.semaphore_signal(
            semaphore, inc=1, device_id={"col": d}, device_id_type=pl.DeviceIdType.MESH)

    for q in range(BANDS):
        @pl.when(band == q)
        def _(q=q):
            pl.semaphore_wait(barrier, (
                2 * quarter - 1, 2 * quarter - 1 + (quarter // 2 if relayed else quarter), half,
                n - 1 - (quarter // 2 if relayed else 0))[q])
            if q == 1:
                tell(near, me - quarter)
                if relayed:
                    tell(near, (seat + quarter // 2) % quarter)
                else:
                    tell(near, me + quarter)
            if q == 3:
                if relayed:
                    for first in (0, half):
                        tell(far, first + seat)
                        tell(far, first + (seat + quarter // 2) % quarter)
                else:
                    for step in range(1, BANDS):
                        tell(far, me - step * quarter)

    def spread(t, rows):
        wide[:, pl.ds(t, 1), :] = rows.astype(jnp.float32)[:, None, :]

    def burst(count, pack_one, copy_one):
        for i in range(count):
            pack_one(i)
            if i:
                copy_one(i - 1).start()
        copy_one(count - 1).start()

    def own_band(first):
        peer = [band * quarter + (seat + j) % quarter for j in range(quarter)]
        for j in range(quarter):
            pack(first + j, peer[j])
        for j in range(1, quarter):
            copy(first + j, peer[j], me).start()

    def send_to(first, dest):
        burst(quarter, lambda j: pack(first + j, dest * quarter + j),
              lambda j: copy(first + j, dest * quarter + j, me))

    def take_from(src):
        copy(0, src, src).wait_recv()
        spread(src, arrived[src])

    def take_own():
        for j in range(1, quarter):
            take_from(band * quarter + (seat + j) % quarter)

    def sent(k, source=None, sems=None):
        copy(k, me, me, source, sems).wait_send()

    if relayed:
        tail = -(-(blocks - MOST * (groups - 1)) * PLEV // TILE) * TILE
        mirror = jnp.where(band == 1, me + quarter, me - quarter)

        def stage_copies(t):
            first, last = STAGES[t], min(STAGES[t + 1], groups)
            spans = [pl.ds(first, last - first)] if last < groups else [
                pl.ds(first, last - 1 - first), (groups - 1, pl.ds(0, tail))]
            return [
                pltpu.make_async_remote_copy(
                    src_ref=queued.at[span], dst_ref=lists[t].at[span],
                    send_sem=queue_sem.at[2 * t + i], recv_sem=queue_sem.at[2 * STEPS + 2 * t + i],
                    device_id={"col": mirror}, device_id_type=pl.DeviceIdType.MESH)
                for i, span in enumerate(spans)
            ]

        def local(j):
            return copy(j, quarter + j, me)

        @pl.when(band == 0)
        def _():
            for j in range(quarter):
                pack(j, quarter + j)
                if 0 < j <= EARLY[1]:
                    local(j - 1).start()

            @pl.when(seat < quarter // 2)
            def _():
                for j in range(EARLY[1], EARLY[0]):
                    local(j).start()

        def slot_of(i):
            return i if i < quarter else i + quarter

        def spell(order):
            return [p * quarter + a * quarter // 4 + i for p, a in order for i in range(quarter // 4)]

        @pl.when(band == 3)
        def _():
            dests = spell(CROSS[1])
            burst(len(dests), lambda i: pack(slot_of(i), dests[i]), lambda i: copy(slot_of(i), dests[i], me))
            pl.semaphore_wait(near, 1)

        @pl.when(inner)
        def _():
            for g in range(groups):
                fill(queued.at[g], res, queue[MOST * g:MOST * g + MOST],
                     ROWS if g < groups - 1 else tail)
                for t in range(STEPS - 1):
                    if g == STAGES[t + 1]:
                        for c in stage_copies(t):
                            c.start()
            for c in stage_copies(STEPS - 1):
                c.start()

            @pl.when(band == 2)
            def _():
                pl.semaphore_wait(far, 2)
                tell(near, me + quarter)

            send_to(0, jnp.where(band == 1, 0, 3))

        own_band(OWN_AT * quarter)
        spread(me, packed[OWN_AT * quarter])

        def take_edge(place, j):
            take_from(jnp.where(band == 0, EDGE_TAKE[0][place], EDGE_TAKE[1][place]) * quarter + j)

        @pl.when(band == 0)
        def _():
            pl.semaphore_wait(near, 2)
            pl.semaphore_wait(far, 2)

            @pl.when(seat >= quarter // 2)
            def _():
                for j in range(EARLY[1], EARLY[0]):
                    local(j).start()

            for j in range(EARLY[0], quarter):
                local(j).start()
            dests = spell(CROSS[0])
            burst(half, lambda i: pack(half + i, dests[i]), lambda i: copy(half + i, dests[i], me))

        @pl.when(jnp.logical_not(inner))
        def _():
            take_own()

            for place in range(1, BANDS):
                for j in range(quarter):
                    take_edge(place, j)
            for k in range(2 * quarter, 4 * quarter):
                sent(k)

        @pl.when(inner)
        def _():
            outer = jnp.where(band == 1, 0, 3)
            peers = [outer * quarter + j for j in range(quarter)]
            peers += [band * quarter + (seat + j) % quarter for j in range(1, quarter)]
            peers += [me]
            where = [locate(d) for d in peers]
            def pass_on(i):
                return copy(i, peers[i], mirror, again, again_sem)

            for t in range(STEPS):
                for c in stage_copies(t):
                    c.wait_recv()
                for g in range(STAGES[t]):
                    lists[t][g] = lists[t - 1][g]
                if t < STEPS - 1:
                    @pl.when(band == 1)
                    def _(t=t):
                        for i in range(STAGES[t], STAGES[t + 1]):
                            fill(again.at[i], lists[t], [
                                jnp.where(w == groups, STAGES[t + 1], w) for w in where[i]])
                        for i in range(STAGES[t], STAGES[t + 1]):
                            pass_on(i).start()

            @pl.when(band == 2)
            def _():
                for i in range(STAGES[STEPS - 1]):
                    fill(again.at[i], lists[STEPS - 1], where[i])
                    if i:
                        pass_on(i - 1).start()
                pass_on(STAGES[STEPS - 1] - 1).start()

            for i in range(STAGES[STEPS - 1], half):
                fill(again.at[i], lists[STEPS - 1], where[i])
                if i > STAGES[STEPS - 1]:
                    pass_on(i - 1).start()
            take_own()
            for j in range(quarter):
                take_from(outer * quarter + j)
            spread(mirror, again[half - 1])
            for j in range(1, quarter):
                take_from((BANDS - 1 - band) * quarter + (seat + j) % quarter)
            for j in range(quarter):
                take_from((BANDS - 1 - outer) * quarter + j)
            for t in range(STEPS):
                for c in stage_copies(t):
                    c.wait_send()
            for i in range(half - 1):
                sent(i, again, again_sem)

        for k in range(quarter):
            sent(k)
        for k in range(OWN_AT * quarter + 1, (OWN_AT + 1) * quarter):
            sent(k)
    else:
        send_band(0)

        @pl.when(band == 0)
        def _():
            pl.semaphore_wait(near, 1)

        send_band(1)

        @pl.when(band == 2)
        def _():
            pl.semaphore_wait(near, 1)

        send_band(2)

        @pl.when(band < 3)
        def _():
            pl.semaphore_wait(far, 1)

        send_band(3)

        spread(me, packed[OWN * quarter])

        def take(place):
            def one(j):
                src = choose(TAKE, place, band) * quarter + ((seat + quarter - j) % quarter if place == 0 else j)
                copy(0, src, src).wait_recv()
                spread(src, arrived[src])

            loop(1 if place == 0 else 0, quarter, one)

        for place in range(BANDS):
            take(place)

        loop(0, OWN * quarter, sent)
        loop(OWN * quarter + 1, n, sent)

    turn = places(me)[2] if relayed else jnp.int32(0)
    for s in range(MOST):
        series[s] = wide[pl.ds(shift(s, turn) * PLEV, PLEV)].astype(jnp.bfloat16)


def close(tm, series, tm_out, series_out, sems):
    first = pltpu.make_async_copy(series, series_out, sems.at[0])
    second = pltpu.make_async_copy(tm, tm_out, sems.at[1])
    first.start()
    second.start()
    first.wait()
    second.wait()


def per_device(fields, level_count, owner, band_start, interp_weights):
    n = lax.axis_size("col")
    blocks = owner.shape[0]
    anywhere = pl.BlockSpec(memory_space=pl.ANY)
    cols = blocks * CBLK
    vmem = pl.BlockSpec(memory_space=pltpu.VMEM)
    grant = 2 * cols * TALL + 2 * CBLK * ROWS * (blocks + 1 + 2 * n) + 4 * CBLK * n * ROWS
    grant += blocks * CBLK * 4 * 16 + 2 * cols * 48 + 2 * n * ROWS * CBLK + blocks * WIDE * 512 + (3 << 20)
    grant += 2 * (blocks + n) * ROWS * CBLK
    timemajor, series = pl.pallas_call(
        functools.partial(kernel, n, blocks),
        out_shape=(
            jax.ShapeDtypeStruct((1, PLEV, cols), jnp.bfloat16),
            jax.ShapeDtypeStruct((MOST, PLEV, n, CBLK), jnp.bfloat16),
        ),
        in_specs=[pl.BlockSpec(memory_space=pltpu.HBM)] * 5,
        out_specs=(vmem, vmem),
        scratch_shapes=[
            pltpu.VMEM((LEV, cols), jnp.bfloat16),
            pltpu.VMEM((blocks, CBLK), jnp.int32),
            pltpu.SMEM((blocks,), jnp.int32),
            pltpu.VMEM((blocks, PLEV), jnp.int32),
            pltpu.VMEM((blocks * BAND, PLEV), jnp.float32),
            pltpu.VMEM((blocks, CBLK), jnp.float32),
            pltpu.VMEM((blocks * BAND, CBLK), jnp.float32),
            pltpu.VMEM((blocks, WIDE, LEV), jnp.bfloat16),
            pltpu.VMEM((blocks + 1, ROWS, CBLK), jnp.bfloat16),
            pltpu.VMEM((n, ROWS, CBLK), jnp.bfloat16),
            pltpu.VMEM((n, ROWS, CBLK), jnp.bfloat16),
            pltpu.VMEM((ROWS, n, CBLK), jnp.float32),
            pltpu.SemaphoreType.DMA((len(CUTS) - 1,)),
            pltpu.SemaphoreType.DMA((4,)),
            pltpu.SemaphoreType.DMA((n,)),
            pltpu.SemaphoreType.DMA((n,)),
            pltpu.SemaphoreType.REGULAR,
            pltpu.SemaphoreType.REGULAR,
            pltpu.VMEM((-(-blocks // MOST), ROWS, CBLK), jnp.bfloat16),
            pltpu.VMEM((n // 2, ROWS, CBLK), jnp.bfloat16),
            pltpu.SemaphoreType.DMA((4 * STEPS,)),
            pltpu.SemaphoreType.DMA((n // 2,)),
            pltpu.SMEM((blocks + MOST,), jnp.int32),
            *[pltpu.VMEM((min(last, -(-blocks // MOST)) + 1, ROWS, CBLK), jnp.bfloat16) for last in STAGES[1:]],
        ],
        compiler_params=pltpu.CompilerParams(
            collective_id=0, has_side_effects=True, vmem_limit_bytes=grant
        ),
    )(
        *[pltpu.with_memory_space_constraint(x, pltpu.HBM) for x in (
            fields, level_count.reshape(blocks, CBLK), owner, band_start,
            jnp.swapaxes(interp_weights, 1, 2).reshape(blocks * BAND, PLEV),
        )]
    )
    return pl.pallas_call(
        close,
        out_shape=(
            jax.ShapeDtypeStruct((1, PLEV, cols), jnp.bfloat16),
            jax.ShapeDtypeStruct((MOST, PLEV, n, CBLK), jnp.bfloat16),
        ),
        in_specs=[vmem, vmem],
        out_specs=(anywhere, anywhere),
        scratch_shapes=[pltpu.SemaphoreType.DMA((2,))],
        compiler_params=pltpu.CompilerParams(vmem_limit_bytes=3 << 20),
    )(timemajor, series)


def solution(mesh):
    placed = (P(("groups", "col"), None, None), P(), P(), P(), P())
    return jax.shard_map(
        per_device,
        mesh=mesh,
        in_specs=placed,
        out_specs=(P(("groups", "col"), None, None), P(("groups", "col"), None, None, None)),
        check_vma=False,
    )
```

```python
import functools

import jax
import jax.numpy as jnp
from jax import lax
from jax.experimental import pallas as pl
from jax.experimental.pallas import tpu as pltpu
from jax.sharding import PartitionSpec as P

LEV = 137
PLEV = 37
BAND = 4
CBLK = 128
MOST = 3
TILE = 16
LOW = (LEV // 2 - 1) // TILE * TILE
TALL = -(-LEV // TILE) * TILE
ROWS = -(-MOST * PLEV // TILE) * TILE
WIDE = -(-PLEV // TILE) * TILE
BANDS = 4
CUTS = (0, 16)
SEND = ((1, 2, 0, 3), (2, 0, 1, 3), (0, 1, 2, 3), (0, 2, 3, 1))
OWN = 2
TAKE = ((0, 3, 2, 1), (1, 0, 3, 2), (2, 3, 0, 1), (3, 2, 0, 1))
OWN_AT = 1
EARLY = (4, 3)
CROSS = (((3, 0), (3, 1), (3, 2), (3, 3), (2, 0), (2, 1), (2, 2), (2, 3)),
         ((2, 0), (2, 1), (2, 2), (2, 3), (0, 0), (0, 1), (1, 0), (0, 2), (0, 3), (1, 1), (1, 2), (1, 3)))
EDGE_TAKE = ((0, 1, 3, 2), (3, 2, 0, 1))
STAGES = (0, 2, 4, 1 << 20)
STEPS = len(STAGES) - 1


def loop(first, last, body):
    if last - first <= 16:
        for i in range(first, last):
            body(i)
    else:

        def step(i, carry):
            body(i)
            return carry

        lax.fori_loop(first, last, step, 0)


def choose(table, place, band):
    value = jnp.int32(table[0][place])
    for q in range(1, BANDS):
        value = jnp.where(band == q, jnp.int32(table[q][place]), value)
    return value


def kernel(n, blocks, fields, counts_in, owner_in, starts_in, weights_in, tm, series,
           data, counts, owner, starts, weights, start_row, weight_row, matrix, res, packed, arrived, wide,
           load_sem, small_sem, send_sem, recv_sem, near, far, queued, again, queue_sem, again_sem, line, *lists):
    me = lax.axis_index("col")
    half = n // 2
    quarter = n // BANDS
    band = me // quarter
    seat = me % quarter
    barrier = pltpu.get_barrier_semaphore()

    smalls = []
    for i, (src, dst) in enumerate(
        [(owner_in, owner), (starts_in, starts), (weights_in, weights), (counts_in, counts)]
    ):
        small = pltpu.make_async_copy(src, dst, small_sem.at[i])
        small.start()
        smalls.append(small)
    loads = []
    for i, (first, last) in enumerate(zip(CUTS, CUTS[1:])):
        span = pl.ds(blocks * first // 16 * CBLK, blocks * (last - first) // 16 * CBLK)
        load = pltpu.make_async_copy(fields.at[0, :, span], data.at[:, span], load_sem.at[i])
        load.start()
        loads.append(load)

    relayed = blocks <= 16 and quarter <= 16

    def greet(d):
        pl.semaphore_signal(
            barrier, inc=1, device_id={"col": d}, device_id_type=pl.DeviceIdType.MESH)

    @pl.when(band < 2)
    def _():
        loop(1, n, lambda i: greet((me + i) % n))

    @pl.when(band == 2)
    def _():
        if relayed:
            loop(0, quarter // 2, lambda i: greet(quarter + seat // (quarter // 2) * (quarter // 2) + i))
        else:
            loop(0, quarter, lambda i: greet(quarter + i))
        loop(0, quarter, lambda i: greet(half + quarter + i))

    @pl.when(band == 3)
    def _():
        if relayed:
            part = seat // (quarter // 2) * (quarter // 2)
            loop(1, quarter // 2, lambda i: greet(half + quarter + part + (seat + i) % (quarter // 2)))
        else:
            loop(1, quarter, lambda i: greet(half + quarter + (seat + i) % quarter))

    res[blocks] = jnp.zeros(res.shape[1:], jnp.bfloat16)
    for part in lists:
        part[part.shape[0] - 1] = jnp.zeros(part.shape[1:], jnp.bfloat16)
    for small in smalls[:-1]:
        small.wait()

    start_row[...] = jnp.concatenate(
        [starts[...].astype(jnp.float32),
         jnp.full((blocks, CBLK - PLEV), -float(CBLK), jnp.float32)], axis=1)
    weight_row[...] = jnp.concatenate(
        [weights[...], jnp.zeros((blocks * BAND, CBLK - PLEV), jnp.float32)], axis=1)

    unit = 1 << blocks.bit_length()
    groups = -(-blocks // MOST)

    def third(x):
        return (x * 43) >> 7

    def shift(c, turn):
        return jnp.where(c + turn >= MOST, c + turn - MOST, c + turn)

    base = (1 - me // half) * half

    def away(d):
        return jnp.where(d < base, d - base + n, d - base)

    if relayed:
        keys = [away(owner[b]) * unit + b for b in range(blocks)]
        before = jnp.int32(0)
        for key in keys:
            before = before + jnp.where(key < half * unit, 1, 0)
        size = 1 << (blocks - 1).bit_length()
        ranked = keys + [jnp.int32(n * unit + blocks)] * (size - blocks)
        p = 1
        while p < size:
            k = p
            while k >= 1:
                for j in range(k % p, size - k, 2 * k):
                    for i in range(min(k, size - j - k)):
                        if (i + j) // (2 * p) == (i + j + k) // (2 * p):
                            x, y = ranked[i + j], ranked[i + j + k]
                            ranked[i + j], ranked[i + j + k] = jnp.minimum(x, y), jnp.maximum(x, y)
                k //= 2
            p *= 2
        ranked = ranked[:blocks]
        for i in range(blocks):
            line[i] = ranked[i]
        for i in range(MOST):
            line[blocks + i] = jnp.int32(n * unit + blocks)
        queue = [key & (unit - 1) for key in ranked] + [jnp.int32(blocks)] * (groups * MOST - blocks)

    def places(d):
        first = jnp.int32(0)
        for key in keys:
            first = first + jnp.where(key < away(d) * unit, 1, 0)
        listed = first - jnp.where(away(d) >= half, before, 0)
        return first, listed, listed - MOST * third(listed)

    def parts(d):
        first, listed, turn = places(d)
        for c in range(MOST):
            step = jnp.where(c >= turn, c - turn, c - turn + MOST)
            key = line[first + step]
            yield key < (away(d) + 1) * unit, key & (unit - 1), listed + step

    def find(d):
        if relayed:
            return [jnp.where(mine, block, blocks) for mine, block, place in parts(d)]

        def look(i, found):
            b = blocks - 1 - i
            return jnp.where(owner[b] == d, found * unit + b, found)

        found = jnp.int32(blocks)
        for s in range(1, MOST):
            found = found * unit + blocks
        if blocks <= 16:
            for i in range(blocks):
                found = look(i, found)
        else:
            found = lax.fori_loop(0, blocks, look, found)
        return [(found // unit ** s) % unit for s in range(MOST)]

    def locate(d):
        return [jnp.where(mine, third(place), groups) for mine, block, place in parts(d)]

    def target(place, j):
        return choose(SEND, place, band) * quarter + ((seat + j) % quarter if place == OWN else j)

    early = None
    if relayed:
        inner = (band == 1) | (band == 2)
    elif quarter <= 16:
        early = [find(target(0, j)) for j in range(quarter)]

    row = lax.broadcasted_iota(jnp.int32, (TILE, CBLK), 0).astype(jnp.float32).astype(jnp.bfloat16)
    zero = jnp.zeros((TILE, CBLK), jnp.bfloat16)

    def packed_row(ref, i):
        return jnp.broadcast_to(ref[pl.ds(i, 1), :], (TILE, CBLK)).astype(jnp.bfloat16)

    def build(b):
        first = packed_row(start_row, b)
        terms = [packed_row(weight_row, b * BAND + k) for k in range(BAND)]
        parts = []
        for i in range(0, TALL, TILE):
            offset = (row + float(i)) - first
            part = zero
            for k in range(BAND):
                part = jnp.where(offset == float(k), terms[k], part)
            parts.append(part)
        matrix[b] = jnp.concatenate(parts, axis=0).T[:WIDE, :LEV]

    loop(0, blocks, build)

    def interpolate(b):
        cols = pl.ds(pl.multiple_of(b * CBLK, CBLK), CBLK)
        count = jnp.broadcast_to(
            counts[pl.ds(b, 1), :].astype(jnp.float32), (TILE, CBLK)).astype(jnp.bfloat16)
        filled = [data[:LOW, cols]]
        last = zero
        ends = 0.0
        for i in range(LOW, LEV, TILE):
            size = min(TILE, LEV - i)
            part = jnp.where(row[:size] + float(i + 1) == count[:size], data[i:i + size, cols], zero[:size])
            if size == TILE:
                last = last + part
            else:
                ends = jnp.sum(part.astype(jnp.float32), axis=0, keepdims=True)
        last = jnp.sum(last.astype(jnp.float32), axis=0, keepdims=True) + ends
        last = jnp.broadcast_to(last, (TILE, CBLK)).astype(jnp.bfloat16)
        for i in range(LOW, LEV, TILE):
            size = min(TILE, LEV - i)
            filled.append(jnp.where(row[:size] + float(i) < count[:size], data[i:i + size, cols], last[:size]))
        out = jnp.dot(
            matrix[b], jnp.concatenate(filled, axis=0), preferred_element_type=jnp.float32)[:PLEV]
        tm[0, :, cols] = out.astype(jnp.bfloat16)
        res[b] = jnp.concatenate(
            [out] * MOST + [jnp.zeros((ROWS - MOST * PLEV, CBLK), jnp.float32)], axis=0,
        ).astype(jnp.bfloat16)

    for small in smalls[-1:]:
        small.wait()
    for load, first, last in zip(loads, CUTS, CUTS[1:]):
        load.wait()
        loop(blocks * first // 16, blocks * last // 16, interpolate)

    def fill(target, source, where, rows=ROWS):
        for i in range(0, rows, TILE):
            slots = [s for s in range(MOST) if s * PLEV < i + TILE and (s + 1) * PLEV > i]
            part = source[where[slots[0]], pl.ds(i, TILE)]
            for s in slots[1:]:
                part = jnp.where(
                    row < float(s * PLEV - i), part, source[where[s], pl.ds(i, TILE)])
            target[pl.ds(i, TILE)] = part

    def pack(k, d, where=None):
        fill(packed.at[k], res, find(d) if where is None else where)

    def copy(k, src_dst, slot, source=None, sems=None):
        return pltpu.make_async_remote_copy(
            src_ref=(packed if source is None else source).at[k], dst_ref=arrived.at[slot],
            send_sem=(send_sem if sems is None else sems).at[k], recv_sem=recv_sem.at[slot],
            device_id={"col": src_dst}, device_id_type=pl.DeviceIdType.MESH,
        )

    def send_band(place):
        def one(j):
            pack(place * quarter + j, target(place, j))

            @pl.when(j > 0)
            def _():
                copy(place * quarter + j - 1, target(place, j - 1), me).start()

        if place != OWN:
            if quarter <= 16:
                for j in range(quarter):
                    pack(place * quarter + j, target(place, j), None if place else early[j])
                    if j:
                        copy(place * quarter + j - 1, target(place, j - 1), me).start()
            else:
                loop(0, quarter, one)
            copy((place + 1) * quarter - 1, target(place, quarter - 1), me).start()
        else:
            def local(j):
                pack(place * quarter + j, target(place, j))

            loop(0, quarter, local)

            def send(j):
                copy(place * quarter + j, target(place, j), me).start()

            loop(1, quarter, send)

    def tell(semaphore, d):
        pl.semaphore_signal(
            semaphore, inc=1, device_id={"col": d}, device_id_type=pl.DeviceIdType.MESH)

    for q in range(BANDS):
        @pl.when(band == q)
        def _(q=q):
            pl.semaphore_wait(barrier, (
                2 * quarter - 1, 2 * quarter - 1 + (quarter // 2 if relayed else quarter), half,
                n - 1 - (quarter // 2 if relayed else 0))[q])
            if q == 1:
                tell(near, me - quarter)
                if relayed:
                    tell(near, (seat + quarter // 2) % quarter)
                else:
                    tell(near, me + quarter)
            if q == 3:
                if relayed:
                    for first in (0, half):
                        tell(far, first + seat)
                        tell(far, first + (seat + quarter // 2) % quarter)
                else:
                    for step in range(1, BANDS):
                        tell(far, me - step * quarter)

    def spread(t, rows):
        wide[:, pl.ds(t, 1), :] = rows.astype(jnp.float32)[:, None, :]

    def burst(count, pack_one, copy_one):
        for i in range(count):
            pack_one(i)
            if i:
                copy_one(i - 1).start()
        copy_one(count - 1).start()

    def own_band(first):
        peer = [band * quarter + (seat + j) % quarter for j in range(quarter)]
        for j in range(quarter):
            pack(first + j, peer[j])
        for j in range(1, quarter):
            copy(first + j, peer[j], me).start()

    def send_to(first, dest):
        burst(quarter, lambda j: pack(first + j, dest * quarter + j),
              lambda j: copy(first + j, dest * quarter + j, me))

    def take_from(src):
        copy(0, src, src).wait_recv()
        spread(src, arrived[src])

    def take_own():
        for j in range(1, quarter):
            take_from(band * quarter + (seat + j) % quarter)

    def sent(k, source=None, sems=None):
        copy(k, me, me, source, sems).wait_send()

    if relayed:
        tail = -(-(blocks - MOST * (groups - 1)) * PLEV // TILE) * TILE
        mirror = jnp.where(band == 1, me + quarter, me - quarter)

        def stage_copies(t):
            first, last = STAGES[t], min(STAGES[t + 1], groups)
            spans = [pl.ds(first, last - first)] if last < groups else [
                pl.ds(first, last - 1 - first), (groups - 1, pl.ds(0, tail))]
            return [
                pltpu.make_async_remote_copy(
                    src_ref=queued.at[span], dst_ref=lists[t].at[span],
                    send_sem=queue_sem.at[2 * t + i], recv_sem=queue_sem.at[2 * STEPS + 2 * t + i],
                    device_id={"col": mirror}, device_id_type=pl.DeviceIdType.MESH)
                for i, span in enumerate(spans)
            ]

        def local(j):
            return copy(j, quarter + j, me)

        @pl.when(band == 0)
        def _():
            for j in range(quarter):
                pack(j, quarter + j)
                if 0 < j <= EARLY[1]:
                    local(j - 1).start()

            @pl.when(seat < quarter // 2)
            def _():
                for j in range(EARLY[1], EARLY[0]):
                    local(j).start()

        def slot_of(i):
            return i if i < quarter else i + quarter

        def spell(order):
            swap = (me % 2) * (quarter // 4)
            return [p * quarter + a * quarter // 4 + i + swap * (1 - 2 * (a % 2))
                    for p, a in order for i in range(quarter // 4)]

        @pl.when(band == 3)
        def _():
            dests = spell(CROSS[1])
            burst(len(dests), lambda i: pack(slot_of(i), dests[i]), lambda i: copy(slot_of(i), dests[i], me))
            pl.semaphore_wait(near, 1)

        @pl.when(inner)
        def _():
            for g in range(groups):
                fill(queued.at[g], res, queue[MOST * g:MOST * g + MOST],
                     ROWS if g < groups - 1 else tail)
                for t in range(STEPS - 1):
                    if g == STAGES[t + 1]:
                        for c in stage_copies(t):
                            c.start()
            for c in stage_copies(STEPS - 1):
                c.start()

            @pl.when(band == 2)
            def _():
                pl.semaphore_wait(far, 2)
                tell(near, me + quarter)

            send_to(0, jnp.where(band == 1, 0, 3))

        own_band(OWN_AT * quarter)
        spread(me, packed[OWN_AT * quarter])

        def take_edge(place, j):
            take_from(jnp.where(band == 0, EDGE_TAKE[0][place], EDGE_TAKE[1][place]) * quarter + j)

        @pl.when(band == 0)
        def _():
            pl.semaphore_wait(near, 2)
            pl.semaphore_wait(far, 2)

            @pl.when(seat >= quarter // 2)
            def _():
                for j in range(EARLY[1], EARLY[0]):
                    local(j).start()

            for j in range(EARLY[0], quarter):
                local(j).start()
            dests = spell(CROSS[0])
            burst(half, lambda i: pack(half + i, dests[i]), lambda i: copy(half + i, dests[i], me))

        @pl.when(jnp.logical_not(inner))
        def _():
            take_own()

            for place in range(1, BANDS):
                for j in range(quarter):
                    take_edge(place, j)
            for k in range(2 * quarter, 4 * quarter):
                sent(k)

        @pl.when(inner)
        def _():
            outer = jnp.where(band == 1, 0, 3)
            peers = [outer * quarter + j for j in range(quarter)]
            peers += [band * quarter + (seat + j) % quarter for j in range(1, quarter)]
            peers += [me]
            where = [locate(d) for d in peers]
            def pass_on(i):
                return copy(i, peers[i], mirror, again, again_sem)

            for t in range(STEPS):
                for c in stage_copies(t):
                    c.wait_recv()
                for g in range(STAGES[t]):
                    lists[t][g] = lists[t - 1][g]
                if t < STEPS - 1:
                    @pl.when(band == 1)
                    def _(t=t):
                        for i in range(STAGES[t], STAGES[t + 1]):
                            fill(again.at[i], lists[t], [
                                jnp.where(w == groups, STAGES[t + 1], w) for w in where[i]])
                        for i in range(STAGES[t], STAGES[t + 1]):
                            pass_on(i).start()

            @pl.when(band == 2)
            def _():
                for i in range(STAGES[STEPS - 1]):
                    fill(again.at[i], lists[STEPS - 1], where[i])
                    if i:
                        pass_on(i - 1).start()
                pass_on(STAGES[STEPS - 1] - 1).start()

            for i in range(STAGES[STEPS - 1], half):
                fill(again.at[i], lists[STEPS - 1], where[i])
                if i > STAGES[STEPS - 1]:
                    pass_on(i - 1).start()
            take_own()
            for j in range(quarter):
                take_from(outer * quarter + j)
            spread(mirror, again[half - 1])
            for j in range(1, quarter):
                take_from((BANDS - 1 - band) * quarter + (seat + j) % quarter)
            for j in range(quarter):
                take_from((BANDS - 1 - outer) * quarter + j)
            for t in range(STEPS):
                for c in stage_copies(t):
                    c.wait_send()
            for i in range(half - 1):
                sent(i, again, again_sem)

        for k in range(quarter):
            sent(k)
        for k in range(OWN_AT * quarter + 1, (OWN_AT + 1) * quarter):
            sent(k)
    else:
        send_band(0)

        @pl.when(band == 0)
        def _():
            pl.semaphore_wait(near, 1)

        send_band(1)

        @pl.when(band == 2)
        def _():
            pl.semaphore_wait(near, 1)

        send_band(2)

        @pl.when(band < 3)
        def _():
            pl.semaphore_wait(far, 1)

        send_band(3)

        spread(me, packed[OWN * quarter])

        def take(place):
            def one(j):
                src = choose(TAKE, place, band) * quarter + ((seat + quarter - j) % quarter if place == 0 else j)
                copy(0, src, src).wait_recv()
                spread(src, arrived[src])

            loop(1 if place == 0 else 0, quarter, one)

        for place in range(BANDS):
            take(place)

        loop(0, OWN * quarter, sent)
        loop(OWN * quarter + 1, n, sent)

    turn = places(me)[2] if relayed else jnp.int32(0)
    for s in range(MOST):
        series[s] = wide[pl.ds(shift(s, turn) * PLEV, PLEV)].astype(jnp.bfloat16)


def close(tm, series, tm_out, series_out, sems):
    first = pltpu.make_async_copy(series, series_out, sems.at[0])
    second = pltpu.make_async_copy(tm, tm_out, sems.at[1])
    first.start()
    second.start()
    first.wait()
    second.wait()


def per_device(fields, level_count, owner, band_start, interp_weights):
    n = lax.axis_size("col")
    blocks = owner.shape[0]
    anywhere = pl.BlockSpec(memory_space=pl.ANY)
    cols = blocks * CBLK
    vmem = pl.BlockSpec(memory_space=pltpu.VMEM)
    grant = 2 * cols * TALL + 2 * CBLK * ROWS * (blocks + 1 + 2 * n) + 4 * CBLK * n * ROWS
    grant += blocks * CBLK * 4 * 16 + 2 * cols * 48 + 2 * n * ROWS * CBLK + blocks * WIDE * 512 + (3 << 20)
    grant += 2 * (blocks + n) * ROWS * CBLK
    timemajor, series = pl.pallas_call(
        functools.partial(kernel, n, blocks),
        out_shape=(
            jax.ShapeDtypeStruct((1, PLEV, cols), jnp.bfloat16),
            jax.ShapeDtypeStruct((MOST, PLEV, n, CBLK), jnp.bfloat16),
        ),
        in_specs=[pl.BlockSpec(memory_space=pltpu.HBM)] * 5,
        out_specs=(vmem, vmem),
        scratch_shapes=[
            pltpu.VMEM((LEV, cols), jnp.bfloat16),
            pltpu.VMEM((blocks, CBLK), jnp.int32),
            pltpu.SMEM((blocks,), jnp.int32),
            pltpu.VMEM((blocks, PLEV), jnp.int32),
            pltpu.VMEM((blocks * BAND, PLEV), jnp.float32),
            pltpu.VMEM((blocks, CBLK), jnp.float32),
            pltpu.VMEM((blocks * BAND, CBLK), jnp.float32),
            pltpu.VMEM((blocks, WIDE, LEV), jnp.bfloat16),
            pltpu.VMEM((blocks + 1, ROWS, CBLK), jnp.bfloat16),
            pltpu.VMEM((n, ROWS, CBLK), jnp.bfloat16),
            pltpu.VMEM((n, ROWS, CBLK), jnp.bfloat16),
            pltpu.VMEM((ROWS, n, CBLK), jnp.float32),
            pltpu.SemaphoreType.DMA((len(CUTS) - 1,)),
            pltpu.SemaphoreType.DMA((4,)),
            pltpu.SemaphoreType.DMA((n,)),
            pltpu.SemaphoreType.DMA((n,)),
            pltpu.SemaphoreType.REGULAR,
            pltpu.SemaphoreType.REGULAR,
            pltpu.VMEM((-(-blocks // MOST), ROWS, CBLK), jnp.bfloat16),
            pltpu.VMEM((n // 2, ROWS, CBLK), jnp.bfloat16),
            pltpu.SemaphoreType.DMA((4 * STEPS,)),
            pltpu.SemaphoreType.DMA((n // 2,)),
            pltpu.SMEM((blocks + MOST,), jnp.int32),
            *[pltpu.VMEM((min(last, -(-blocks // MOST)) + 1, ROWS, CBLK), jnp.bfloat16) for last in STAGES[1:]],
        ],
        compiler_params=pltpu.CompilerParams(
            collective_id=0, has_side_effects=True, vmem_limit_bytes=grant
        ),
    )(
        *[pltpu.with_memory_space_constraint(x, pltpu.HBM) for x in (
            fields, level_count.reshape(blocks, CBLK), owner, band_start,
            jnp.swapaxes(interp_weights, 1, 2).reshape(blocks * BAND, PLEV),
        )]
    )
    return pl.pallas_call(
        close,
        out_shape=(
            jax.ShapeDtypeStruct((1, PLEV, cols), jnp.bfloat16),
            jax.ShapeDtypeStruct((MOST, PLEV, n, CBLK), jnp.bfloat16),
        ),
        in_specs=[vmem, vmem],
        out_specs=(anywhere, anywhere),
        scratch_shapes=[pltpu.SemaphoreType.DMA((2,))],
        compiler_params=pltpu.CompilerParams(vmem_limit_bytes=3 << 20),
    )(timemajor, series)


def solution(mesh):
    placed = (P(("groups", "col"), None, None), P(), P(), P(), P())
    return jax.shard_map(
        per_device,
        mesh=mesh,
        in_specs=placed,
        out_specs=(P(("groups", "col"), None, None), P(("groups", "col"), None, None, None)),
        check_vma=False,
    )
```
